128 devices in a mesh: seq: 32 (over x, z, core), head: 4 (over y).
Axes of the slice: x: 4, y: 4, z: 4, core: 2. Of those that a mesh axis runs over, the one named last changes fastest.
Arguments:
- queries: bfloat16 [24576, 8192], P('seq', 'head'), may hold values from -6 to 6
- key_rows: bfloat16 [24576, 8192], P('seq', 'head'), may hold values from -0.5 to 0.5
- value_rows: bfloat16 [24576, 8192], P('seq', 'head'), may hold values from -130 to 130
- log_decay: float32 [64, 24576], P('head', 'seq'), may hold values from -1 to 0
- norm_gain: float32 [8192], P('head'), may hold values from 0.1 to 1.9
- grad_out: bfloat16 [24576, 8192], P('seq', 'head'), may hold values from -13 to 13
Outputs:
- output: bfloat16 [24576, 8192], P('seq', 'head')
- grad_queries: bfloat16 [24576, 8192], P('seq', 'head')
- grad_keys: bfloat16 [24576, 8192], P('seq', 'head')
- grad_values: bfloat16 [24576, 8192], P('seq', 'head')
- grad_gain: float32 [8192], P('head')
The draws below stay inside these ranges and needn't reach their ends.
All inputs are finite; a program needn't handle non-finite values.
Results may differ from the reference program's by a relative error of at most 0.01.
Values sent between devices are 32-bit elements; how exact they have to be, the bound alone decides.
A program may use at most 192 MiB of HBM per device.

```python
import jax
import jax.numpy as jnp
from jax import lax

HEADS = 64
DH = 128
TOK_DEV = 768
SEQUENCE_TOKENS = 24576
HD = 8192


def draw_log_decay(key, part):
    sample_sequences = jax.random.split(key, 6)
    token_position = jnp.arange(SEQUENCE_TOKENS)
    fast_share = 0.5
    picked = jax.random.uniform(sample_sequences[0], (HEADS, 1), dtype=jnp.float32)
    fast_rate = jnp.exp(jax.random.uniform(sample_sequences[1], (HEADS, 1), dtype=jnp.float32, minval=jnp.log(1.0 / 50.0), maxval=jnp.log(1.0 / 30.0)))
    slow_rate = 0.6 / SEQUENCE_TOKENS
    baseline_decay_rate = jnp.where(picked < fast_share, fast_rate, slow_rate)
    block_count = SEQUENCE_TOKENS // TOK_DEV
    block_multiplier = jnp.exp(jax.random.uniform(sample_sequences[2], (HEADS, block_count), dtype=jnp.float32, minval=jnp.log(0.5), maxval=jnp.log(2.0)))
    block_multiplier = jnp.repeat(block_multiplier, TOK_DEV, axis=1, total_repeat_length=SEQUENCE_TOKENS)
    jitter_amplitude = jax.random.uniform(sample_sequences[3], (HEADS, SEQUENCE_TOKENS), dtype=jnp.float32, minval=0.5, maxval=1.5)
    spike_locations = jax.random.randint(sample_sequences[4], (3,), 0, SEQUENCE_TOKENS)
    spike_magnitude = jax.random.uniform(sample_sequences[5], (HEADS, 3), dtype=jnp.float32, minval=0.22, maxval=0.69)
    decay_spikes = jnp.sum(jnp.where(token_position[None, :, None] == spike_locations[None, None, :], spike_magnitude[:, None, :], 0.0), axis=2)
    return (-(baseline_decay_rate * block_multiplier * jitter_amplitude + decay_spikes)).astype(jnp.float32)


def draw_value_rows(key, part):
    sample_sequences = jax.random.split(key, 3)
    head_number = (jnp.arange(HD) // DH).astype(jnp.float32)
    head_scale = 1.0 + 2.0 * head_number / max(HEADS - 1, 1)
    base = jnp.clip(jax.random.normal(sample_sequences[0], (SEQUENCE_TOKENS, HD), dtype=jnp.float32), -4.0, 4.0)
    row_scale = jnp.exp(jax.random.uniform(sample_sequences[2], (SEQUENCE_TOKENS, 1), dtype=jnp.float32, minval=0.0, maxval=jnp.log(10.0)))
    return (base * head_scale[None, :] * row_scale).astype(jnp.bfloat16)


def draw_grad_out(key, part):
    sample_sequences = jax.random.split(key, 1)
    ramp = 1.0 + 2.0 * jnp.arange(SEQUENCE_TOKENS).astype(jnp.float32) / (SEQUENCE_TOKENS - 1)
    base = jnp.clip(jax.random.normal(sample_sequences[0], (SEQUENCE_TOKENS, HD), dtype=jnp.float32), -4.0, 4.0)
    return (base * ramp[:, None]).astype(jnp.bfloat16)


def level_of(rng, dims, cuts, least, largest):
    def one(axis_at, parts):
        draws = jax.random.uniform(jax.random.fold_in(jax.random.fold_in(rng, 6), axis_at), (parts,), jnp.float32, least / len(cuts), largest / len(cuts))
        return jnp.repeat(jnp.exp(draws), dims[axis_at] // parts).reshape((-1,) + (1,) * (len(dims) - axis_at - 1))

    factor_of = one(*cuts[0])
    for cut in cuts[1:]:
        factor_of = factor_of * one(*cut)
    return factor_of


def normal_values(rng, extent, width, limit, cuts=(), held_as=jnp.bfloat16):
    result = jax.random.normal(rng, extent, jnp.float32) * width
    if len(cuts) > 0:
        result = level_of(rng, extent, cuts, -0.22, 0.18) * result
    return jnp.clip(result, min=-limit, max=limit).astype(held_as)


def setup_inputs(seed: int = 0) -> dict:
    arg_keys = jax.random.split(jax.random.key(seed), 7)
    queries = normal_values(arg_keys[0], (SEQUENCE_TOKENS, HD), 1.0, 6.0, ((0, 32), (1, 4)))
    key_rows = normal_values(arg_keys[1], (SEQUENCE_TOKENS, HD), DH ** -0.5, 0.5, ((0, 32), (1, 4)))
    value_rows = draw_value_rows(jax.random.fold_in(arg_keys[6], 71), 0)
    log_decay = draw_log_decay(jax.random.fold_in(arg_keys[6], 71), 0)
    norm_gain = jnp.clip(1.0 + 0.18 * jax.random.normal(arg_keys[4], (HD,), jnp.float32), 0.1, 1.9)
    grad_out = draw_grad_out(jax.random.fold_in(arg_keys[6], 71), 0)
    return dict(queries=queries, key_rows=key_rows, value_rows=value_rows, log_decay=log_decay, norm_gain=norm_gain, grad_out=grad_out)


EPSILON = 1e-06

def exact_product(form, left, right):
    return jnp.einsum(form, left.astype(jnp.float32), right.astype(jnp.float32), precision=lax.Precision.HIGHEST)

def plain_product(form, left, right):
    return jnp.einsum(form, left.astype(jnp.float32), right.astype(jnp.float32))

def causal_decay(cumulative):
    length = cumulative.shape[-1]
    below_diag = jnp.arange(length)[:, None] >= jnp.arange(length)[None, :]
    spread = cumulative[..., :, None] - cumulative[..., None, :]
    return jnp.where(below_diag, jnp.exp(jnp.where(below_diag, spread, 0.0)), 0.0)

def split_heads(matrix):
    return matrix.reshape(matrix.shape[0], HEADS, DH).transpose(1, 0, 2)

def merge_heads(tensor):
    return tensor.transpose(1, 0, 2).reshape(tensor.shape[1], HD)

def attend(q_heads, k_heads, v_heads, cumulative, state):
    decay_mask = causal_decay(cumulative)
    scores = plain_product('htd,hsd->hts', q_heads, k_heads)
    weights = (scores * decay_mask).astype(jnp.bfloat16)
    attended = plain_product('hts,hsd->htd', weights, v_heads)
    attended = attended + jnp.exp(cumulative)[..., None] * exact_product('htd,hde->hte', q_heads, state)
    return (attended, weights, decay_mask)

def normalize(attended, grad_rows, norm_gain):
    mixed = merge_heads(attended)
    inverse = lax.rsqrt(lax.optimization_barrier(jnp.mean(mixed * mixed, axis=1)) + EPSILON)
    normed = mixed * inverse[:, None]
    scaled = grad_rows.astype(jnp.float32) * norm_gain[None, :]
    center = lax.optimization_barrier(jnp.mean(scaled * normed, axis=1))
    grad_attended = (inverse[:, None] * (scaled - normed * center[:, None])).astype(jnp.bfloat16)
    return (normed, split_heads(grad_attended))

def reference(queries, key_rows, value_rows, log_decay, norm_gain, grad_out):
    blocks = SEQUENCE_TOKENS // TOK_DEV

    def tile(matrix):
        return matrix.reshape(blocks, TOK_DEV, HEADS, DH).transpose(0, 2, 1, 3)
    q_all = tile(queries)
    k_all = tile(key_rows)
    v_all = tile(value_rows)
    grad_rows = grad_out.reshape(blocks, TOK_DEV, HD)
    cumulative = jnp.cumsum(log_decay.reshape(HEADS, blocks, TOK_DEV).transpose(1, 0, 2), axis=2)
    block_total = cumulative[:, :, -1]

    def local_fn(operands):
        k_heads, v_heads, cumul, last_value = operands
        tail = jnp.exp(last_value[:, None] - cumul)
        return exact_product('htd,hte->hde', k_heads.astype(jnp.float32) * tail[..., None], v_heads)
    local_state = lax.map(local_fn, (k_all, v_all, cumulative, block_total))

    def carry_step(carry, operands):
        decay_total, local_term = operands
        return (decay_total[:, None, None] * carry + local_term, carry)
    zero_state = jnp.zeros((HEADS, DH, DH), jnp.float32)
    _, state_in = lax.scan(carry_step, zero_state, (jnp.exp(block_total), local_state))

    def second_pass(operands):
        q_heads, k_heads, v_heads, grad_block, cumul, state = operands
        attended, _, _ = attend(q_heads, k_heads, v_heads, cumul, state)
        normed, grad_heads = normalize(attended, grad_block, norm_gain)
        output_block = (normed * norm_gain[None, :]).astype(jnp.bfloat16)
        gain_part = lax.optimization_barrier(jnp.sum(grad_block.astype(jnp.float32) * normed, axis=0))
        state_grad = exact_product('htd,hte->hde', q_heads.astype(jnp.float32) * jnp.exp(cumul)[..., None], grad_heads)
        return (output_block, gain_part, state_grad)
    output, gain_parts, state_grad = lax.map(second_pass, (q_all, k_all, v_all, grad_rows, cumulative, state_in))
    _, state_after = lax.scan(carry_step, zero_state, (jnp.exp(block_total), state_grad), reverse=True)

    def fourth_pass(operands):
        q_heads, k_heads, v_heads, grad_block, cumul, last_value, state, after = operands
        attended, weights, decay_mask = attend(q_heads, k_heads, v_heads, cumul, state)
        _, grad_heads = normalize(attended, grad_block, norm_gain)
        grad_weights = (plain_product('htd,hsd->hts', grad_heads, v_heads) * decay_mask).astype(jnp.bfloat16)
        tail = jnp.exp(last_value[:, None] - cumul)[..., None]
        grad_q = plain_product('hts,hsd->htd', grad_weights, k_heads)
        grad_q = grad_q + jnp.exp(cumul)[..., None] * exact_product('hte,hde->htd', grad_heads, state)
        grad_k = plain_product('hts,htd->hsd', grad_weights, q_heads)
        grad_k = grad_k + tail * exact_product('hse,hde->hsd', v_heads, after)
        grad_v = plain_product('hts,htd->hsd', weights, grad_heads)
        grad_v = grad_v + tail * exact_product('hsd,hde->hse', k_heads, after)
        return (merge_heads(grad_q).astype(jnp.bfloat16), merge_heads(grad_k).astype(jnp.bfloat16), merge_heads(grad_v).astype(jnp.bfloat16))
    grad_q, grad_k, grad_v = lax.map(fourth_pass, (q_all, k_all, v_all, grad_rows, cumulative, block_total, state_in, state_after))
    grad_gain = lax.optimization_barrier(jnp.sum(gain_parts, axis=0))
    return (output.reshape(SEQUENCE_TOKENS, HD), grad_q.reshape(SEQUENCE_TOKENS, HD), grad_k.reshape(SEQUENCE_TOKENS, HD), grad_v.reshape(SEQUENCE_TOKENS, HD), grad_gain)
```

```python
import functools

import jax
import jax.numpy as jnp
from jax import lax
from jax.experimental import pallas as pl
from jax.experimental.pallas import tpu as pltpu
from jax.sharding import PartitionSpec as P

DH = 128
EPSILON = 1e-06
F32 = jnp.float32
BF16 = jnp.bfloat16
MESH = pl.DeviceIdType.MESH
HIGHEST = lax.Precision.HIGHEST


def nn(a, b):
    return lax.dot_general(a, b, (((1,), (0,)), ((), ())), preferred_element_type=F32)


def nt(a, b):
    return lax.dot_general(a, b, (((1,), (1,)), ((), ())), preferred_element_type=F32)


def tn(a, b):
    return lax.dot_general(a, b, (((0,), (0,)), ((), ())), preferred_element_type=F32)


def exact_nt(a, b):
    return lax.dot_general(
        a, b, (((1,), (1,)), ((), ())), preferred_element_type=F32, precision=HIGHEST
    )


def kernel(
    sizes,
    q_in, k_in, v_in, ld, gain, g_in,
    out_hbm, gq_hbm, gk_hbm, gv_hbm, gg_out,
    q, k, v, g, cb, rc, ms, att, gvi, sbf, ga, qt,
    acc_s, acc_c, invb, cenb, sums, hx,
    dec_own, dec_par, dec_chip, dec_all,
    loc, lpr, tot, rx, px, pin, st, pst,
    gloc, glpr, gtot, grx, gpx, gpin, gst, gpst,
    ggp, ggpr, ggc, ggrx, ggsum, ggall,
    in_sem, out_sem, dp_s, dp_r, da_s, da_r, hx_s, hx_r,
    lp_s, lp_r, rx_s, rx_r, pi_s, pi_r, ps_s, ps_r,
    glp_s, glp_r, grx_s, grx_r, gpi_s, gpi_r, gps_s, gps_r,
    gp_s, gp_r, gr_s, gr_r, ga_s, ga_r,
):
    T, H, NC, NY = sizes
    NJ = T // DH
    HH = H // 2
    RS = HH * DH // NC
    HD = NY * H * DH
    me = lax.axis_index("seq")
    y = lax.axis_index("head")
    chip = me // 2
    core = me % 2
    mate = chip * 2 + (1 - core)
    own0 = core * HH
    oth0 = (1 - core) * HH

    def at(i):
        return {"seq": i * 2 + core}

    def remote(src, dst, s, r, dev):
        return pltpu.make_async_remote_copy(
            src_ref=src, dst_ref=dst, send_sem=s, recv_sem=r, device_id=dev, device_id_type=MESH
        )

    def loop(n, body):
        lax.fori_loop(0, n, lambda i, c: (body(i), c)[1], 0)

    def others(body):
        lax.fori_loop(1, NC, lambda r, c: (body(lax.rem(chip + r, NC)), c)[1], 0)

    loads = [
        pltpu.make_async_copy(src, dst, in_sem.at[n])
        for n, (src, dst) in enumerate(((k_in, k), (v_in, v), (q_in, q), (g_in, g)))
    ]
    for c in loads:
        c.start()

    barrier = pltpu.get_barrier_semaphore()
    others(
        lambda i: pl.semaphore_signal(barrier, inc=1, device_id=at(i), device_id_type=MESH)
    )
    pl.semaphore_signal(barrier, inc=1, device_id={"seq": mate}, device_id_type=MESH)
    for r in range(1, NY):
        pl.semaphore_signal(
            barrier, inc=1, device_id={"head": lax.rem(y + r, NY)}, device_id_type=MESH
        )

    row_i = lax.broadcasted_iota(jnp.int32, (DH, DH), 0)
    col_i = lax.broadcasted_iota(jnp.int32, (DH, DH), 1)
    lower = row_i >= col_i
    upper = row_i <= col_i
    tri = jnp.where(lower, 1.0, 0.0).astype(F32)

    total = jnp.zeros((H, 1), F32)
    for j in range(NJ):
        piece = ld[:, j * DH:(j + 1) * DH]
        rows = exact_nt(piece, tri)
        columns = exact_nt(tri, piece)
        for h in range(H):
            rc[h, :, j * DH:(j + 1) * DH] = rows[h:h + 1, :]
            cb[h, j * DH:(j + 1) * DH, :] = jnp.broadcast_to(columns[:, h:h + 1], (DH, DH))
        total = total + rows[:, DH - 1:DH]
    dec_own[...] = jnp.broadcast_to(total, (H, DH)).reshape(H, 1, DH)

    pl.semaphore_wait(barrier, NC - 1 + 1 + NY - 1)
    dec_copy = remote(dec_own, dec_par, dp_s.at[0], dp_r.at[0], {"seq": mate})
    dec_copy.start()

    def tile(ref, h, j):
        return ref[j * DH:(j + 1) * DH, pl.ds(pl.multiple_of(h * DH, DH), DH)]

    def put(ref, h, j, value):
        ref[j * DH:(j + 1) * DH, pl.ds(pl.multiple_of(h * DH, DH), DH)] = value

    def cums(h, j):
        return cb[h, j * DH:(j + 1) * DH, :]

    def cum_row(h, j):
        return rc[h, :, j * DH:(j + 1) * DH]

    def local_states(h):
        state = None
        for j in range(NJ):
            cum = cums(h, j)
            end = cum[DH - 1:DH, :]
            scaled = (tile(k, h, j).astype(F32) * jnp.exp(end - cum)).astype(BF16)
            part = tn(scaled, tile(v, h, j))
            ms[h, j] = part
            state = part if state is None else jnp.exp(end) * state + part
        loc[h] = state

    def to_mate(src, dst, s, r, n):
        return remote(src, dst, s.at[n], r.at[n], {"seq": mate})

    def scan_total(first, src, recv, dst):
        def one(r):
            h = own0 + r
            mine = jnp.where(first, jnp.exp(dec_par[h]), 1.0)
            theirs = jnp.where(first, 1.0, jnp.exp(dec_own[h]))
            dst[pl.ds(pl.multiple_of(r * DH, DH), DH), :] = mine * src[h] + theirs * recv[r]

        loop(HH, one)

    def piece_of(ref, i):
        return ref.at[pl.ds(pl.multiple_of(i * RS, RS), RS), :]

    def out_copy(src, dst, s, r, i):
        return remote(piece_of(src, i), dst.at[chip], s.at[i], r.at[chip], at(i))

    def in_copy(src, dst, s, r, i):
        return remote(piece_of(src, i), dst.at[i], s.at[i], r.at[i], at(i))

    def back_copy(src, dst, s, r, i):
        return remote(src.at[i], piece_of(dst, chip), s.at[i], r.at[chip], at(i))

    def home_copy(src, dst, s, r, i):
        return remote(src.at[i], piece_of(dst, i), s.at[i], r.at[i], at(i))

    def prefix(src, recv, dst, s, r, reverse):
        head = own0 + (chip * RS) // DH
        recv[chip] = src[pl.ds(pl.multiple_of(chip * RS, RS), RS), :]

        def one(n, state):
            i = NC - 1 - n if reverse else n

            @pl.when(i != chip)
            def _():
                in_copy(src, recv, s, r, i).wait_recv()

            dst[i] = state
            return jnp.exp(dec_all[i, head]) * state + recv[i]

        lax.fori_loop(0, NC, one, jnp.zeros((RS, DH), F32))

    def settle(first, homed, local, recv, dst, out):
        def one(r):
            h = own0 + r
            state = homed[pl.ds(pl.multiple_of(r * DH, DH), DH), :]
            ahead = jnp.where(first, 1.0, jnp.exp(dec_par[h]))
            dst[h] = ahead * state + jnp.where(first, 0.0, recv[r])
            after = jnp.where(first, jnp.exp(dec_own[h]), 1.0)
            out[r] = after * state + jnp.where(first, local[h], 0.0)

        loop(HH, one)

    loads[0].wait()
    loads[1].wait()

    def first_half(r):
        local_states(oth0 + r)
        to_mate(loc.at[oth0 + r], lpr.at[r], lp_s, lp_r, r).start()

    loop(HH, first_half)
    dec_copy.wait()
    dec_chip[...] = dec_own[...] + dec_par[...]
    dec_all[chip] = dec_chip[...]
    others(lambda i: remote(dec_chip, dec_all.at[chip], da_s.at[i], da_r.at[chip], at(i)).start())
    loop(HH, lambda r: local_states(own0 + r))
    loop(HH, lambda r: to_mate(loc.at[oth0 + r], lpr.at[r], lp_s, lp_r, r).wait())
    scan_total(core == 0, loc, lpr, tot)
    others(lambda i: out_copy(tot, rx, rx_s, rx_r, i).start())

    loads[2].wait()

    def intra(h):
        for j in range(NJ):
            qj = tile(q, h, j)
            decay = jnp.exp(jnp.where(lower, cums(h, j) - cum_row(h, j), -jnp.inf))
            weights = (nt(qj, tile(k, h, j)) * decay).astype(BF16)
            put(att, h, j, nn(weights, tile(v, h, j)))
            qt[h, :, j * DH:(j + 1) * DH] = qj.T

    loop(HH, intra)
    others(lambda i: remote(dec_chip, dec_all.at[i], da_s.at[i], da_r.at[i], at(i)).wait())
    prefix(tot, rx, px, rx_s, rx_r, False)
    others(lambda i: back_copy(px, pin, pi_s, pi_r, i).start())
    pin[pl.ds(pl.multiple_of(chip * RS, RS), RS), :] = px[chip]
    loop(HH, lambda r: intra(HH + r))
    loads[3].wait()
    acc_s[...] = jnp.zeros_like(acc_s)
    acc_c[...] = jnp.zeros_like(acc_c)
    others(lambda i: home_copy(px, pin, pi_s, pi_r, i).wait_recv())
    settle(core == 0, pin, loc, lpr, st, pst)
    loop(HH, lambda r: to_mate(pst.at[r], st.at[own0 + r], ps_s, ps_r, r).start())

    def inter(h):
        state = st[h]
        scale = gain[:, pl.ds(pl.multiple_of(h * DH, DH), DH)]
        for j in range(NJ):
            cum = cums(h, j)
            low = state.astype(BF16)
            sbf[h, j] = low
            mixed = tile(att, h, j) + jnp.exp(cum) * nn(tile(q, h, j), low)
            put(att, h, j, mixed)
            acc_s[j * DH:(j + 1) * DH, :] += mixed * mixed
            acc_c[j * DH:(j + 1) * DH, :] += tile(g, h, j).astype(F32) * scale * mixed
            if j < NJ - 1:
                state = jnp.exp(cum[DH - 1:DH, :]) * state + ms[h, j]

    loop(HH, lambda r: inter(own0 + r))

    def second_half(r):
        to_mate(pst.at[r], st.at[oth0 + r], ps_s, ps_r, r).wait_recv()
        inter(oth0 + r)

    loop(HH, second_half)

    ones = jnp.ones((8, DH), F32)
    pick = lax.broadcasted_iota(jnp.int32, (8, DH), 0) == 0
    for j in range(NJ):
        a = exact_nt(ones, acc_s[j * DH:(j + 1) * DH, :])
        b = exact_nt(ones, acc_c[j * DH:(j + 1) * DH, :])
        sums[:, j * DH:(j + 1) * DH] = jnp.where(pick, a, b)
    for r in range(1, NY):
        d = lax.rem(y + r, NY)
        remote(sums, hx.at[y], hx_s.at[d], hx_r.at[y], {"head": d}).start()
    hx[y] = sums[...]
    for r in range(1, NY):
        d = lax.rem(y + r, NY)
        remote(sums, hx.at[d], hx_s.at[d], hx_r.at[d], {"head": d}).wait()
    for j in range(NJ):
        both = hx[0, :, j * DH:(j + 1) * DH]
        for r in range(1, NY):
            both = both + hx[r, :, j * DH:(j + 1) * DH]
        both = both.T
        inverse = lax.rsqrt(both[:, 0:1] / HD + EPSILON)
        center = both[:, 1:2] * inverse / HD
        invb[j * DH:(j + 1) * DH, :] = jnp.broadcast_to(inverse, (DH, DH))
        cenb[j * DH:(j + 1) * DH, :] = jnp.broadcast_to(center, (DH, DH))

    def normalize(h):
        scale = gain[:, pl.ds(pl.multiple_of(h * DH, DH), DH)]
        gain_part = jnp.zeros((8, DH), F32)
        for j in range(NJ):
            inverse = invb[j * DH:(j + 1) * DH, :]
            normed = tile(att, h, j) * inverse
            grad = tile(g, h, j).astype(F32)
            put(g, h, j, (normed * scale).astype(BF16))
            gain_part = gain_part + jnp.sum((grad * normed).reshape(DH // 8, 8, DH), axis=0)
            center = cenb[j * DH:(j + 1) * DH, :]
            low = (inverse * (grad * scale - normed * center)).astype(BF16)
            put(ga, h, j, low)
            lifted = qt[h, :, j * DH:(j + 1) * DH].astype(F32) * jnp.exp(cum_row(h, j))
            ms[h, j] = nn(lifted.astype(BF16), low)
        ggp[h] = gain_part
        state = ms[h, NJ - 1]
        for j in range(NJ - 2, -1, -1):
            end = cb[h, j * DH + DH - 1:j * DH + DH, :]
            state = jnp.exp(end) * state + ms[h, j]
        gloc[h] = state

    def normalize_send(r):
        normalize(oth0 + r)
        to_mate(gloc.at[oth0 + r], glpr.at[r], glp_s, glp_r, r).start()

    loop(HH, normalize_send)
    loop(HH, lambda r: normalize(own0 + r))
    gain_copy = to_mate(ggp, ggpr, gp_s, gp_r, 0)
    gain_copy.start()
    store_out = pltpu.make_async_copy(g, out_hbm, out_sem.at[0])
    store_out.start()
    loop(HH, lambda r: to_mate(gloc.at[oth0 + r], glpr.at[r], glp_s, glp_r, r).wait())
    scan_total(core == 1, gloc, glpr, gtot)
    others(lambda i: out_copy(gtot, grx, grx_s, grx_r, i).start())
    gain_copy.wait()
    ggc[...] = ggp[...] + ggpr[...]
    others(lambda i: remote(ggc.at[i], ggrx.at[chip], gr_s.at[i], gr_r.at[chip], at(i)).start())
    ggrx[chip] = ggc[chip]

    def intra_grads(h):
        for j in range(NJ):
            qj, kj, vj, gj = (tile(ref, h, j) for ref in (q, k, v, ga))
            cum = cums(h, j)
            row = cum_row(h, j)
            decay = jnp.exp(jnp.where(lower, cum - row, -jnp.inf))
            flipped = jnp.exp(jnp.where(upper, row - cum, -jnp.inf))
            gw = (nt(gj, vj) * decay).astype(BF16)
            gwt = (nt(vj, gj) * flipped).astype(BF16)
            wt = (nt(kj, qj) * flipped).astype(BF16)
            gq = nn(gw, kj) + jnp.exp(cum) * nt(gj, sbf[h, j])
            put(att, h, j, nn(gwt, qj))
            put(gvi, h, j, nn(wt, gj))
            put(q, h, j, gq.astype(BF16))

    loop(HH, intra_grads)
    prefix(gtot, grx, gpx, grx_s, grx_r, True)
    others(lambda i: back_copy(gpx, gpin, gpi_s, gpi_r, i).start())
    gpin[pl.ds(pl.multiple_of(chip * RS, RS), RS), :] = gpx[chip]
    others(lambda i: remote(ggc.at[i], ggrx.at[i], gr_s.at[i], gr_r.at[i], at(i)).wait())
    part = ggrx[0]
    for i in range(1, NC):
        part = part + ggrx[i]
    ggsum[...] = part
    others(lambda i: remote(ggsum, ggall.at[chip], ga_s.at[i], ga_r.at[chip], at(i)).start())
    ggall[chip] = part
    loop(HH, lambda r: intra_grads(HH + r))
    store_q = pltpu.make_async_copy(q, gq_hbm, out_sem.at[1])
    store_q.start()
    others(lambda i: home_copy(gpx, gpin, gpi_s, gpi_r, i).wait_recv())
    settle(core == 1, gpin, gloc, glpr, gst, gpst)
    loop(HH, lambda r: to_mate(gpst.at[r], gst.at[own0 + r], gps_s, gps_r, r).start())

    def inter_grads(h):
        state = gst[h]
        for j in range(NJ - 1, -1, -1):
            cum = cums(h, j)
            end = cum[DH - 1:DH, :]
            low = state.astype(BF16)
            tail = jnp.exp(end - cum)
            kj, vj = tile(k, h, j), tile(v, h, j)
            gk = tile(att, h, j) + tail * nt(vj, low)
            gv = tile(gvi, h, j) + tail * nn(kj, low)
            put(k, h, j, gk.astype(BF16))
            put(v, h, j, gv.astype(BF16))
            if j > 0:
                state = jnp.exp(end) * state + ms[h, j]

    loop(HH, lambda r: inter_grads(own0 + r))

    def grads_half(r):
        to_mate(gpst.at[r], gst.at[oth0 + r], gps_s, gps_r, r).wait_recv()
        inter_grads(oth0 + r)

    loop(HH, grads_half)
    store_k = pltpu.make_async_copy(k, gk_hbm, out_sem.at[2])
    store_k.start()
    store_v = pltpu.make_async_copy(v, gv_hbm, out_sem.at[3])
    store_v.start()
    others(lambda i: remote(ggsum, ggall.at[i], ga_s.at[i], ga_r.at[i], at(i)).wait())
    for h in range(H):
        gg_out[h:h + 1, :] = jnp.sum(ggall[h], axis=0, keepdims=True)

    others(lambda i: in_copy(tot, rx, rx_s, rx_r, i).wait_send())
    others(lambda i: home_copy(px, pin, pi_s, pi_r, i).wait_send())
    others(lambda i: in_copy(gtot, grx, grx_s, grx_r, i).wait_send())
    others(lambda i: home_copy(gpx, gpin, gpi_s, gpi_r, i).wait_send())
    loop(HH, lambda r: to_mate(pst.at[r], st.at[oth0 + r], ps_s, ps_r, r).wait_send())
    loop(HH, lambda r: to_mate(gpst.at[r], gst.at[oth0 + r], gps_s, gps_r, r).wait_send())
    for c in (store_out, store_q, store_k, store_v):
        c.wait()


def on_device(sizes, queries, key_rows, value_rows, log_decay, norm_gain, grad_out):
    T, H, NC, NY = sizes
    W = H * DH
    NJ = T // DH
    HH = H // 2
    RS = HH * DH // NC
    V = pltpu.VMEM
    D = pltpu.SemaphoreType.DMA
    mate_scan = [
        V((H, DH, DH), F32), V((HH, DH, DH), F32), V((HH * DH, DH), F32), V((NC, RS, DH), F32),
        V((NC, RS, DH), F32), V((HH * DH, DH), F32), V((H, DH, DH), F32), V((HH, DH, DH), F32),
    ]
    scan_sems = [D((HH,)), D((HH,)), D((NC,)), D((NC,)), D((NC,)), D((NC,)), D((HH,)), D((HH,))]
    scratch = [
        V((T, W), BF16), V((T, W), BF16), V((T, W), BF16), V((T, W), BF16),
        V((H, T, DH), F32), V((H, 1, T), F32), V((H, NJ, DH, DH), F32), V((T, W), F32),
        V((T, W), F32), V((H, NJ, DH, DH), BF16), V((T, W), BF16), V((H, DH, T), BF16),
        V((T, DH), F32), V((T, DH), F32), V((T, DH), F32), V((T, DH), F32),
        V((8, T), F32), V((NY, 8, T), F32),
        V((H, 1, DH), F32), V((H, 1, DH), F32), V((H, 1, DH), F32), V((NC, H, 1, DH), F32),
        *mate_scan, *mate_scan,
        V((H, 8, DH), F32), V((H, 8, DH), F32), V((H, 8, DH), F32), V((NC, 8, DH), F32),
        V((8, DH), F32), V((NC, 8, DH), F32),
        D((4,)), D((4,)), D((1,)), D((1,)), D((NC,)), D((NC,)), D((NY,)), D((NY,)),
        *scan_sems, *scan_sems,
        D((1,)), D((1,)), D((NC,)), D((NC,)), D((NC,)), D((NC,)),
    ]
    big = jax.ShapeDtypeStruct((T, W), BF16)
    anywhere = pl.BlockSpec(memory_space=pl.ANY)
    local = pl.BlockSpec(memory_space=pltpu.VMEM)
    *grads, gain_grad = pl.pallas_call(
        functools.partial(kernel, sizes),
        out_shape=(big, big, big, big, jax.ShapeDtypeStruct((H, DH), F32)),
        in_specs=[anywhere, anywhere, anywhere, local, local, anywhere],
        out_specs=(anywhere, anywhere, anywhere, anywhere, local),
        scratch_shapes=scratch,
        compiler_params=pltpu.CompilerParams(
            collective_id=0, has_side_effects=True, vmem_limit_bytes=66_000_000
        ),
    )(queries, key_rows, value_rows, log_decay, norm_gain.reshape(1, W), grad_out)
    return (*grads, gain_grad.reshape(W))


def solution(mesh):
    def whole(queries, key_rows, value_rows, log_decay, norm_gain, grad_out):
        seq, head = mesh.shape["seq"], mesh.shape["head"]
        sizes = (queries.shape[0] // seq, queries.shape[1] // DH // head, seq // 2, head)
        rows = P("seq", "head")
        return jax.shard_map(
            functools.partial(on_device, sizes),
            mesh=mesh,
            in_specs=(rows, rows, rows, P("head", "seq"), P("head"), rows),
            out_specs=(rows, rows, rows, rows, P("head")),
            check_vma=False,
        )(queries, key_rows, value_rows, log_decay, norm_gain, grad_out)

    return whole
```

```python
import functools

import jax
import jax.numpy as jnp
from jax import lax
from jax.experimental import pallas as pl
from jax.experimental.pallas import tpu as pltpu
from jax.sharding import PartitionSpec as P

DH = 128
EPSILON = 1e-06
F32 = jnp.float32
BF16 = jnp.bfloat16
MESH = pl.DeviceIdType.MESH
HIGHEST = lax.Precision.HIGHEST


def nn(a, b):
    return lax.dot_general(a, b, (((1,), (0,)), ((), ())), preferred_element_type=F32)


def nt(a, b):
    return lax.dot_general(a, b, (((1,), (1,)), ((), ())), preferred_element_type=F32)


def tn(a, b):
    return lax.dot_general(a, b, (((0,), (0,)), ((), ())), preferred_element_type=F32)


def exact_nt(a, b):
    return lax.dot_general(
        a, b, (((1,), (1,)), ((), ())), preferred_element_type=F32, precision=HIGHEST
    )


def tile(ref, h, j):
    return ref[j * DH:(j + 1) * DH, pl.ds(pl.multiple_of(h * DH, DH), DH)]


def put(ref, h, j, value):
    ref[j * DH:(j + 1) * DH, pl.ds(pl.multiple_of(h * DH, DH), DH)] = value


def inter_grads(sizes, h, to, k, v, cb, sbf, att, gvi, gk, gv):
    for j in range(sizes[0] // DH):
        cum = cb[h, j * DH:(j + 1) * DH, :]
        low = sbf[h, j]
        tail = jnp.exp(cum[DH - 1:DH, :] - cum)
        kj, vj = tile(k, h, j), tile(v, h, j)
        put(gk, to, j, (tile(att, h, j) + tail * nt(vj, low)).astype(BF16))
        put(gv, to, j, (tile(gvi, h, j) + tail * nn(kj, low)).astype(BF16))


def finish(
    sizes,
    q, k, v, g, cb, sbf, att, gvi, gg,
    out_hbm, gq_hbm, gk_hbm, gv_hbm, gg_out,
    gk, gv, sem, head_sem,
):
    HH = sizes[1] // 2
    HW = HH * DH
    core = lax.axis_index("seq") % 2
    own = pl.ds(pl.multiple_of(core * HW, HW), HW)
    copies = [
        pltpu.make_async_copy(src, dst, sem.at[n])
        for n, (src, dst) in enumerate((
            (g, out_hbm), (q, gq_hbm),
            (k.at[:, own], gk_hbm.at[:, own]), (v.at[:, own], gv_hbm.at[:, own]),
        ))
    ]
    for c in copies:
        c.start()
    gg_out[...] = gg[...]

    def stores(r):
        src = pl.ds(pl.multiple_of(r * DH, DH), DH)
        dst = pl.ds(pl.multiple_of(((1 - core) * HH + r) * DH, DH), DH)
        return [
            pltpu.make_async_copy(a.at[:, src], b.at[:, dst], head_sem.at[n, r])
            for n, (a, b) in enumerate(((gk, gk_hbm), (gv, gv_hbm)))
        ]

    def one(r, carry):
        inter_grads(sizes, (1 - core) * HH + r, r, k, v, cb, sbf, att, gvi, gk, gv)
        for c in stores(r):
            c.start()
        return carry

    lax.fori_loop(0, HH, one, 0)
    for r in range(HH):
        for c in stores(r):
            c.wait()
    for c in copies:
        c.wait()


def kernel(
    sizes,
    q_in, k_in, v_in, ld, gain, g_in,
    q, k, v, g, cb, sbf, att, gvi, gg_out,
    rc, ms, ga,
    acc_s, acc_c, invb, cenb, sums, hx,
    dec_own, dec_par, dec_chip, dec_all,
    loc, lpr, tot, rx, px, pin, st, pst,
    gloc, glpr, gtot, grx, gpx, gpin, gst, gpst,
    ggp, ggpr, ggc, ggrx, ggsum, ggall,
    in_sem, dp_s, dp_r, da_s, da_r, hx_s, hx_r,
    lp_s, lp_r, rx_s, rx_r, pi_s, pi_r, ps_s, ps_r,
    glp_s, glp_r, grx_s, grx_r, gpi_s, gpi_r, gps_s, gps_r,
    gp_s, gp_r, gr_s, gr_r, ga_s, ga_r,
):
    T, H, NC, NY = sizes
    NJ = T // DH
    HH = H // 2
    RS = HH * DH // NC
    HD = NY * H * DH
    me = lax.axis_index("seq")
    y = lax.axis_index("head")
    chip = me // 2
    core = me % 2
    mate = chip * 2 + (1 - core)
    own0 = core * HH
    oth0 = (1 - core) * HH

    def at(i):
        return {"seq": i * 2 + core}

    def remote(src, dst, s, r, dev):
        return pltpu.make_async_remote_copy(
            src_ref=src, dst_ref=dst, send_sem=s, recv_sem=r, device_id=dev, device_id_type=MESH
        )

    def loop(n, body):
        lax.fori_loop(0, n, lambda i, c: (body(i), c)[1], 0)

    def others(body):
        lax.fori_loop(1, NC, lambda r, c: (body(lax.rem(chip + r, NC)), c)[1], 0)

    loads = [
        pltpu.make_async_copy(src, dst, in_sem.at[n])
        for n, (src, dst) in enumerate(((k_in, k), (v_in, v), (q_in, q), (g_in, g)))
    ]
    for c in loads:
        c.start()

    barrier = pltpu.get_barrier_semaphore()
    others(
        lambda i: pl.semaphore_signal(barrier, inc=1, device_id=at(i), device_id_type=MESH)
    )
    pl.semaphore_signal(barrier, inc=1, device_id={"seq": mate}, device_id_type=MESH)
    for r in range(1, NY):
        pl.semaphore_signal(
            barrier, inc=1, device_id={"head": lax.rem(y + r, NY)}, device_id_type=MESH
        )

    row_i = lax.broadcasted_iota(jnp.int32, (DH, DH), 0)
    col_i = lax.broadcasted_iota(jnp.int32, (DH, DH), 1)
    lower = row_i >= col_i
    upper = row_i <= col_i
    tri = jnp.where(lower, 1.0, 0.0).astype(F32)

    total = jnp.zeros((H, 1), F32)
    for j in range(NJ):
        piece = ld[:, j * DH:(j + 1) * DH]
        rows = exact_nt(piece, tri)
        columns = exact_nt(tri, piece)
        for h in range(H):
            rc[h, :, j * DH:(j + 1) * DH] = rows[h:h + 1, :]
            cb[h, j * DH:(j + 1) * DH, :] = jnp.broadcast_to(columns[:, h:h + 1], (DH, DH))
        total = total + rows[:, DH - 1:DH]
    dec_own[...] = jnp.broadcast_to(total, (H, DH)).reshape(H, 1, DH)

    pl.semaphore_wait(barrier, NC - 1 + 1 + NY - 1)
    dec_copy = remote(dec_own, dec_par, dp_s.at[0], dp_r.at[0], {"seq": mate})
    dec_copy.start()

    def cums(h, j):
        return cb[h, j * DH:(j + 1) * DH, :]

    def cum_row(h, j):
        return rc[h, :, j * DH:(j + 1) * DH]

    def local_states(h):
        state = None
        for j in range(NJ):
            cum = cums(h, j)
            end = cum[DH - 1:DH, :]
            scaled = (tile(k, h, j).astype(F32) * jnp.exp(end - cum)).astype(BF16)
            part = tn(scaled, tile(v, h, j))
            ms[h, j] = part
            state = part if state is None else jnp.exp(end) * state + part
        loc[h] = state

    def to_mate(src, dst, s, r, n):
        return remote(src, dst, s.at[n], r.at[n], {"seq": mate})

    def scan_total(first, src, recv, dst):
        def one(r):
            h = own0 + r
            mine = jnp.where(first, jnp.exp(dec_par[h]), 1.0)
            theirs = jnp.where(first, 1.0, jnp.exp(dec_own[h]))
            dst[pl.ds(pl.multiple_of(r * DH, DH), DH), :] = mine * src[h] + theirs * recv[r]

        loop(HH, one)

    def piece_of(ref, i):
        return ref.at[pl.ds(pl.multiple_of(i * RS, RS), RS), :]

    def out_copy(src, dst, s, r, i):
        return remote(piece_of(src, i), dst.at[chip], s.at[i], r.at[chip], at(i))

    def in_copy(src, dst, s, r, i):
        return remote(piece_of(src, i), dst.at[i], s.at[i], r.at[i], at(i))

    def back_copy(src, dst, s, r, i):
        return remote(src.at[i], piece_of(dst, chip), s.at[i], r.at[chip], at(i))

    def home_copy(src, dst, s, r, i):
        return remote(src.at[i], piece_of(dst, i), s.at[i], r.at[i], at(i))

    def prefix(src, recv, dst, s, r, reverse):
        head = own0 + (chip * RS) // DH
        recv[chip] = src[pl.ds(pl.multiple_of(chip * RS, RS), RS), :]

        def one(n, state):
            i = NC - 1 - n if reverse else n

            @pl.when(i != chip)
            def _():
                in_copy(src, recv, s, r, i).wait_recv()

            dst[i] = state
            return jnp.exp(dec_all[i, head]) * state + recv[i]

        lax.fori_loop(0, NC, one, jnp.zeros((RS, DH), F32))

    def settle(first, homed, local, recv, dst, out):
        def one(r):
            h = own0 + r
            state = homed[pl.ds(pl.multiple_of(r * DH, DH), DH), :]
            ahead = jnp.where(first, 1.0, jnp.exp(dec_par[h]))
            dst[h] = ahead * state + jnp.where(first, 0.0, recv[r])
            after = jnp.where(first, jnp.exp(dec_own[h]), 1.0)
            out[r] = after * state + jnp.where(first, local[h], 0.0)

        loop(HH, one)

    loads[0].wait()
    loads[1].wait()

    def first_half(r):
        local_states(oth0 + r)
        to_mate(loc.at[oth0 + r], lpr.at[r], lp_s, lp_r, r).start()

    loop(HH, first_half)
    dec_copy.wait()
    dec_chip[...] = dec_own[...] + dec_par[...]
    dec_all[chip] = dec_chip[...]
    others(lambda i: remote(dec_chip, dec_all.at[chip], da_s.at[i], da_r.at[chip], at(i)).start())
    loop(HH, lambda r: local_states(own0 + r))
    loop(HH, lambda r: to_mate(loc.at[oth0 + r], lpr.at[r], lp_s, lp_r, r).wait())
    scan_total(core == 0, loc, lpr, tot)
    others(lambda i: out_copy(tot, rx, rx_s, rx_r, i).start())

    loads[2].wait()

    def intra(h):
        for j in range(NJ):
            qj = tile(q, h, j)
            decay = jnp.exp(jnp.where(lower, cums(h, j) - cum_row(h, j), -jnp.inf))
            weights = (nt(qj, tile(k, h, j)) * decay).astype(BF16)
            put(att, h, j, nn(weights, tile(v, h, j)))
            put(gvi, h, j, qj.astype(F32).T)

    loop(HH, intra)
    others(lambda i: remote(dec_chip, dec_all.at[i], da_s.at[i], da_r.at[i], at(i)).wait())
    prefix(tot, rx, px, rx_s, rx_r, False)
    others(lambda i: back_copy(px, pin, pi_s, pi_r, i).start())
    pin[pl.ds(pl.multiple_of(chip * RS, RS), RS), :] = px[chip]
    loop(HH, lambda r: intra(HH + r))
    loads[3].wait()
    acc_s[...] = jnp.zeros_like(acc_s)
    acc_c[...] = jnp.zeros_like(acc_c)
    others(lambda i: home_copy(px, pin, pi_s, pi_r, i).wait_recv())
    settle(core == 0, pin, loc, lpr, st, pst)
    loop(HH, lambda r: to_mate(pst.at[r], st.at[own0 + r], ps_s, ps_r, r).start())

    def inter(h):
        state = st[h]
        scale = gain[:, pl.ds(pl.multiple_of(h * DH, DH), DH)]
        for j in range(NJ):
            cum = cums(h, j)
            low = state.astype(BF16)
            sbf[h, j] = low
            mixed = tile(att, h, j) + jnp.exp(cum) * nn(tile(q, h, j), low)
            put(att, h, j, mixed)
            acc_s[j * DH:(j + 1) * DH, :] += mixed * mixed
            acc_c[j * DH:(j + 1) * DH, :] += tile(g, h, j).astype(F32) * scale * mixed
            if j < NJ - 1:
                state = jnp.exp(cum[DH - 1:DH, :]) * state + ms[h, j]

    loop(HH, lambda r: inter(own0 + r))

    def second_half(r):
        to_mate(pst.at[r], st.at[oth0 + r], ps_s, ps_r, r).wait_recv()
        inter(oth0 + r)

    loop(HH, second_half)

    ones = jnp.ones((8, DH), F32)
    pick = lax.broadcasted_iota(jnp.int32, (8, DH), 0) == 0
    for j in range(NJ):
        a = exact_nt(ones, acc_s[j * DH:(j + 1) * DH, :])
        b = exact_nt(ones, acc_c[j * DH:(j + 1) * DH, :])
        sums[:, j * DH:(j + 1) * DH] = jnp.where(pick, a, b)
    for r in range(1, NY):
        d = lax.rem(y + r, NY)
        remote(sums, hx.at[y], hx_s.at[d], hx_r.at[y], {"head": d}).start()
    hx[y] = sums[...]
    for r in range(1, NY):
        d = lax.rem(y + r, NY)
        remote(sums, hx.at[d], hx_s.at[d], hx_r.at[d], {"head": d}).wait()
    for j in range(NJ):
        both = hx[0, :, j * DH:(j + 1) * DH]
        for r in range(1, NY):
            both = both + hx[r, :, j * DH:(j + 1) * DH]
        both = both.T
        inverse = lax.rsqrt(both[:, 0:1] / HD + EPSILON)
        center = both[:, 1:2] * inverse / HD
        invb[j * DH:(j + 1) * DH, :] = jnp.broadcast_to(inverse, (DH, DH))
        cenb[j * DH:(j + 1) * DH, :] = jnp.broadcast_to(center, (DH, DH))

    def normalize(h):
        scale = gain[:, pl.ds(pl.multiple_of(h * DH, DH), DH)]
        gain_part = jnp.zeros((8, DH), F32)
        for j in range(NJ):
            inverse = invb[j * DH:(j + 1) * DH, :]
            normed = tile(att, h, j) * inverse
            grad = tile(g, h, j).astype(F32)
            put(g, h, j, (normed * scale).astype(BF16))
            gain_part = gain_part + jnp.sum((grad * normed).reshape(DH // 8, 8, DH), axis=0)
            center = cenb[j * DH:(j + 1) * DH, :]
            low = (inverse * (grad * scale - normed * center)).astype(BF16)
            put(ga, h, j, low)
            lifted = tile(gvi, h, j) * jnp.exp(cum_row(h, j))
            ms[h, j] = nn(lifted.astype(BF16), low)
        ggp[h] = gain_part
        state = ms[h, NJ - 1]
        for j in range(NJ - 2, -1, -1):
            end = cb[h, j * DH + DH - 1:j * DH + DH, :]
            state = jnp.exp(end) * state + ms[h, j]
        gloc[h] = state

    def normalize_send(r):
        normalize(oth0 + r)
        to_mate(gloc.at[oth0 + r], glpr.at[r], glp_s, glp_r, r).start()

    loop(HH, normalize_send)
    loop(HH, lambda r: normalize(own0 + r))
    gain_copy = to_mate(ggp, ggpr, gp_s, gp_r, 0)
    gain_copy.start()
    loop(HH, lambda r: to_mate(gloc.at[oth0 + r], glpr.at[r], glp_s, glp_r, r).wait())
    scan_total(core == 1, gloc, glpr, gtot)
    others(lambda i: out_copy(gtot, grx, grx_s, grx_r, i).start())
    gain_copy.wait()
    ggc[...] = ggp[...] + ggpr[...]
    others(lambda i: remote(ggc.at[i], ggrx.at[chip], gr_s.at[i], gr_r.at[chip], at(i)).start())
    ggrx[chip] = ggc[chip]

    def intra_grads(h):
        for j in range(NJ):
            qj, kj, vj, gj = (tile(ref, h, j) for ref in (q, k, v, ga))
            cum = cums(h, j)
            row = cum_row(h, j)
            decay = jnp.exp(jnp.where(lower, cum - row, -jnp.inf))
            flipped = jnp.exp(jnp.where(upper, row - cum, -jnp.inf))
            gw = (nt(gj, vj) * decay).astype(BF16)
            gwt = (nt(vj, gj) * flipped).astype(BF16)
            wt = (nt(kj, qj) * flipped).astype(BF16)
            gq = nn(gw, kj) + jnp.exp(cum) * nt(gj, sbf[h, j])
            put(att, h, j, nn(gwt, qj))
            put(gvi, h, j, nn(wt, gj))
            put(q, h, j, gq.astype(BF16))

    loop(HH, intra_grads)
    prefix(gtot, grx, gpx, grx_s, grx_r, True)
    others(lambda i: back_copy(gpx, gpin, gpi_s, gpi_r, i).start())
    gpin[pl.ds(pl.multiple_of(chip * RS, RS), RS), :] = gpx[chip]
    others(lambda i: remote(ggc.at[i], ggrx.at[i], gr_s.at[i], gr_r.at[i], at(i)).wait())
    part = ggrx[0]
    for i in range(1, NC):
        part = part + ggrx[i]
    ggsum[...] = part
    others(lambda i: remote(ggsum, ggall.at[chip], ga_s.at[i], ga_r.at[chip], at(i)).start())
    ggall[chip] = part
    loop(HH, lambda r: intra_grads(HH + r))
    others(lambda i: home_copy(gpx, gpin, gpi_s, gpi_r, i).wait_recv())
    settle(core == 1, gpin, gloc, glpr, gst, gpst)
    loop(HH, lambda r: to_mate(gpst.at[r], gst.at[own0 + r], gps_s, gps_r, r).start())

    def later_states(h):
        state = gst[h]
        for j in range(NJ - 1, -1, -1):
            sbf[h, j] = state.astype(BF16)
            if j > 0:
                state = jnp.exp(cb[h, j * DH + DH - 1:j * DH + DH, :]) * state + ms[h, j]

    def own_grads(r):
        later_states(own0 + r)
        inter_grads(sizes, own0 + r, own0 + r, k, v, cb, sbf, att, gvi, k, v)

    loop(HH, own_grads)
    loop(HH, lambda r: to_mate(gpst.at[r], gst.at[own0 + r], gps_s, gps_r, r).wait_send())

    def mate_states(r):
        to_mate(gpst.at[r], gst.at[oth0 + r], gps_s, gps_r, r).wait_recv()
        later_states(oth0 + r)

    loop(HH, mate_states)
    others(lambda i: remote(ggsum, ggall.at[i], ga_s.at[i], ga_r.at[i], at(i)).wait())
    for h in range(H):
        gg_out[h:h + 1, :] = jnp.sum(ggall[h], axis=0, keepdims=True)

    others(lambda i: in_copy(tot, rx, rx_s, rx_r, i).wait_send())
    others(lambda i: home_copy(px, pin, pi_s, pi_r, i).wait_send())
    others(lambda i: in_copy(gtot, grx, grx_s, grx_r, i).wait_send())
    others(lambda i: home_copy(gpx, gpin, gpi_s, gpi_r, i).wait_send())
    loop(HH, lambda r: to_mate(pst.at[r], st.at[oth0 + r], ps_s, ps_r, r).wait_send())


def on_device(sizes, queries, key_rows, value_rows, log_decay, norm_gain, grad_out):
    T, H, NC, NY = sizes
    W = H * DH
    NJ = T // DH
    HH = H // 2
    RS = HH * DH // NC
    V = pltpu.VMEM
    D = pltpu.SemaphoreType.DMA
    mate_scan = [
        V((H, DH, DH), F32), V((HH, DH, DH), F32), V((HH * DH, DH), F32), V((NC, RS, DH), F32),
        V((NC, RS, DH), F32), V((HH * DH, DH), F32), V((H, DH, DH), F32), V((HH, DH, DH), F32),
    ]
    scan_sems = [D((HH,)), D((HH,)), D((NC,)), D((NC,)), D((NC,)), D((NC,)), D((HH,)), D((HH,))]
    scratch = [
        V((H, 1, T), F32), V((H, NJ, DH, DH), F32), V((T, W), BF16),
        V((T, DH), F32), V((T, DH), F32), V((T, DH), F32), V((T, DH), F32),
        V((8, T), F32), V((NY, 8, T), F32),
        V((H, 1, DH), F32), V((H, 1, DH), F32), V((H, 1, DH), F32), V((NC, H, 1, DH), F32),
        *mate_scan, *mate_scan,
        V((H, 8, DH), F32), V((H, 8, DH), F32), V((H, 8, DH), F32), V((NC, 8, DH), F32),
        V((8, DH), F32), V((NC, 8, DH), F32),
        D((4,)), D((1,)), D((1,)), D((NC,)), D((NC,)), D((NY,)), D((NY,)),
        *scan_sems, *scan_sems,
        D((1,)), D((1,)), D((NC,)), D((NC,)), D((NC,)), D((NC,)),
    ]
    anywhere = pl.BlockSpec(memory_space=pl.ANY)
    local = pl.BlockSpec(memory_space=V)
    held = (
        V((T, W), BF16), V((T, W), BF16), V((T, W), BF16), V((T, W), BF16),
        V((H, T, DH), F32), V((H, NJ, DH, DH), BF16), V((T, W), F32), V((T, W), F32),
        V((H, DH), F32),
    )
    parts = pl.pallas_call(
        functools.partial(kernel, sizes),
        out_shape=held,
        in_specs=[anywhere, anywhere, anywhere, local, local, anywhere],
        out_specs=(local,) * len(held),
        scratch_shapes=scratch,
        compiler_params=pltpu.CompilerParams(
            collective_id=0, has_side_effects=True, vmem_limit_bytes=24 << 20
        ),
    )(queries, key_rows, value_rows, log_decay, norm_gain.reshape(1, W), grad_out)
    parts = [pltpu.with_memory_space_constraint(x, V) for x in parts]
    big = jax.ShapeDtypeStruct((T, W), BF16)
    *grads, gain_grad = pl.pallas_call(
        functools.partial(finish, sizes),
        out_shape=(big, big, big, big, jax.ShapeDtypeStruct((H, DH), F32)),
        in_specs=[local] * len(held),
        out_specs=(anywhere, anywhere, anywhere, anywhere, local),
        scratch_shapes=[
            V((T, W // 2), BF16), V((T, W // 2), BF16), D((4,)), D((2, HH)),
        ],
        compiler_params=pltpu.CompilerParams(vmem_limit_bytes=5 << 20),
    )(*parts)
    return (*grads, gain_grad.reshape(W))


def solution(mesh):
    def whole(queries, key_rows, value_rows, log_decay, norm_gain, grad_out):
        seq, head = mesh.shape["seq"], mesh.shape["head"]
        sizes = (queries.shape[0] // seq, queries.shape[1] // DH // head, seq // 2, head)
        rows = P("seq", "head")
        return jax.shard_map(
            functools.partial(on_device, sizes),
            mesh=mesh,
            in_specs=(rows, rows, rows, P("head", "seq"), P("head"), rows),
            out_specs=(rows, rows, rows, rows, P("head")),
            check_vma=False,
        )(queries, key_rows, value_rows, log_decay, norm_gain, grad_out)

    return whole
```

```python
import functools

import jax
import jax.numpy as jnp
from jax import lax
from jax.experimental import pallas as pl
from jax.experimental.pallas import tpu as pltpu
from jax.sharding import PartitionSpec as P

DH = 128
EPSILON = 1e-06
F32 = jnp.float32
BF16 = jnp.bfloat16
MESH = pl.DeviceIdType.MESH
HIGHEST = lax.Precision.HIGHEST


def nn(a, b):
    return lax.dot_general(a, b, (((1,), (0,)), ((), ())), preferred_element_type=F32)


def nt(a, b):
    return lax.dot_general(a, b, (((1,), (1,)), ((), ())), preferred_element_type=F32)


def tn(a, b):
    return lax.dot_general(a, b, (((0,), (0,)), ((), ())), preferred_element_type=F32)


def exact_nt(a, b):
    return lax.dot_general(
        a, b, (((1,), (1,)), ((), ())), preferred_element_type=F32, precision=HIGHEST
    )


def tile(ref, h, j):
    return ref[j * DH:(j + 1) * DH, pl.ds(pl.multiple_of(h * DH, DH), DH)]


def put(ref, h, j, value):
    ref[j * DH:(j + 1) * DH, pl.ds(pl.multiple_of(h * DH, DH), DH)] = value


def inter_grads(sizes, h, to, k, v, cb, sbf, att, gvi, gk, gv):
    for j in range(sizes[0] // DH):
        cum = cb[h, j * DH:(j + 1) * DH, :]
        low = sbf[h, j]
        tail = jnp.exp(cum[DH - 1:DH, :] - cum)
        kj, vj = tile(k, h, j), tile(v, h, j)
        put(gk, to, j, (tile(att, h, j) + tail * nt(vj, low)).astype(BF16))
        put(gv, to, j, (tile(gvi, h, j) + tail * nn(kj, low)).astype(BF16))


def finish(
    sizes,
    q, k, v, g, cb, sbf, att, gvi, gg,
    out_hbm, gq_hbm, gk_hbm, gv_hbm, gg_out,
    gk, gv, sem, head_sem,
):
    HH = sizes[1] // 2
    HW = HH * DH
    core = lax.axis_index("seq") % 2
    own = pl.ds(pl.multiple_of(core * HW, HW), HW)
    copies = [
        pltpu.make_async_copy(src, dst, sem.at[n])
        for n, (src, dst) in enumerate((
            (g, out_hbm), (q, gq_hbm),
            (k.at[:, own], gk_hbm.at[:, own]), (v.at[:, own], gv_hbm.at[:, own]),
        ))
    ]
    for c in copies:
        c.start()
    gg_out[...] = gg[...]

    def stores(r):
        src = pl.ds(pl.multiple_of(r * DH, DH), DH)
        dst = pl.ds(pl.multiple_of(((1 - core) * HH + r) * DH, DH), DH)
        return [
            pltpu.make_async_copy(a.at[:, src], b.at[:, dst], head_sem.at[n, r])
            for n, (a, b) in enumerate(((gk, gk_hbm), (gv, gv_hbm)))
        ]

    def one(r, carry):
        inter_grads(sizes, (1 - core) * HH + r, r, k, v, cb, sbf, att, gvi, gk, gv)
        for c in stores(r):
            c.start()
        return carry

    lax.fori_loop(0, HH, one, 0)
    for r in range(HH):
        for c in stores(r):
            c.wait()
    for c in copies:
        c.wait()


def kernel(
    sizes,
    q_in, k_in, v_in, ld, gain, g_in,
    q, k, v, g, cb, sbf, att, gvi, gg_out,
    rc, ms, ga, kt, wt,
    acc_s, acc_c, sums, hx,
    dec_own, dec_par, dec_chip, dec_all,
    loc, tot, px, pst, lpr, rx, pin, st,
    ggp, ggpr, ggc, ggrx, ggsum, ggall,
    in_sem, dp_s, dp_r, da_s, da_r, hx_s, hx_r,
    lp_s, lp_r, rx_s, rx_r, pi_s, pi_r, ps_s, ps_r,
    glp_s, glp_r, grx_s, grx_r, gpi_s, gpi_r, gps_s, gps_r,
    gp_s, gp_r, gr_s, gr_r, ga_s, ga_r,
):
    T, H, NC, NY = sizes
    NJ = T // DH
    HH = H // 2
    HG = HH // 2
    RS = HG * DH // NC
    HD = NY * H * DH
    PAIR = 2 if HG % 2 == 0 else 1
    me = lax.axis_index("seq")
    y = lax.axis_index("head")
    chip = me // 2
    core = me % 2
    mate = {"seq": chip * 2 + (1 - core)}
    own0 = core * HH
    oth0 = (1 - core) * HH

    def at(i):
        return {"seq": i * 2 + core}

    def remote(src, dst, s, r, dev):
        return pltpu.make_async_remote_copy(
            src_ref=src, dst_ref=dst, send_sem=s, recv_sem=r, device_id=dev, device_id_type=MESH
        )

    def loop(n, body):
        lax.fori_loop(0, n, lambda i, c: (body(i), c)[1], 0)

    def others(body):
        lax.fori_loop(1, NC, lambda r, c: (body(lax.rem(chip + r, NC)), c)[1], 0)

    loads = [
        pltpu.make_async_copy(src, dst, in_sem.at[n])
        for n, (src, dst) in enumerate(((k_in, k), (v_in, v), (q_in, q), (g_in, g)))
    ]
    loads[0].start()
    loads[1].start()

    barrier = pltpu.get_barrier_semaphore()
    others(
        lambda i: pl.semaphore_signal(barrier, inc=1, device_id=at(i), device_id_type=MESH)
    )
    pl.semaphore_signal(barrier, inc=1, device_id=mate, device_id_type=MESH)
    for r in range(1, NY):
        pl.semaphore_signal(
            barrier, inc=1, device_id={"head": lax.rem(y + r, NY)}, device_id_type=MESH
        )

    row_i = lax.broadcasted_iota(jnp.int32, (DH, DH), 0)
    col_i = lax.broadcasted_iota(jnp.int32, (DH, DH), 1)
    lower = row_i >= col_i
    tri = jnp.where(lower, 1.0, 0.0).astype(F32)

    total = jnp.zeros((H, 1), F32)
    for j in range(NJ):
        piece = ld[:, j * DH:(j + 1) * DH]
        rows = exact_nt(piece, tri)
        columns = exact_nt(tri, piece)
        for h in range(H):
            rc[h, :, j * DH:(j + 1) * DH] = rows[h:h + 1, :]
            cb[h, j * DH:(j + 1) * DH, :] = jnp.broadcast_to(columns[:, h:h + 1], (DH, DH))
        total = total + rows[:, DH - 1:DH]
    dec_own[...] = jnp.broadcast_to(total, (H, DH)).reshape(H, 1, DH)
    loads[2].start()
    loads[3].start()

    def cums(h, j):
        return cb[h, j * DH:(j + 1) * DH, :]

    def cum_row(h, j):
        return rc[h, :, j * DH:(j + 1) * DH]

    def local_states(h):
        state = None
        for j in range(NJ):
            row = cum_row(h, j)
            end = row[:, DH - 1:DH]
            flipped = tile(k, h, j).T
            put(kt, h, j, flipped)
            scaled = (flipped.astype(F32) * jnp.exp(end - row)).astype(BF16)
            part = nn(scaled, tile(v, h, j))
            ms[h, j] = part
            last = jnp.exp(cb[h, j * DH + DH - 1:j * DH + DH, :])
            state = part if state is None else last * state + part
        loc[h] = state

    def group(ref, base, n):
        return ref.at[pl.ds(base + n * HG, HG)]

    def swap(src, recv, s, r, n):
        return remote(group(src, oth0, n), recv.at[n], s.at[n], r.at[n], mate)

    def give(dst, s, r, n, base):
        return remote(pst.at[n], group(dst, base, n), s.at[n], r.at[n], mate)

    def scan_total(first, recv, n):
        def one(r):
            h = own0 + n * HG + r
            mine = jnp.where(first, jnp.exp(dec_par[h]), 1.0)
            theirs = jnp.where(first, 1.0, jnp.exp(dec_own[h]))
            tot[n, pl.ds(pl.multiple_of(r * DH, DH), DH), :] = mine * loc[h] + theirs * recv[n, r]

        loop(HG, one)

    def piece_of(ref, n, i):
        return ref.at[n, pl.ds(pl.multiple_of(i * RS, RS), RS), :]

    def send_out(recv, s, r, n):
        others(
            lambda i: remote(piece_of(tot, n, i), recv.at[n, chip], s.at[n], r.at[n], at(i)).start()
        )

    def all_out(recv, s, r, n):
        return remote(
            tot.at[n, pl.ds(0, (NC - 1) * RS), :], tot.at[n, pl.ds(0, (NC - 1) * RS), :],
            s.at[n], r.at[n], mate,
        )

    def all_in(recv, s, r, n):
        part = recv.at[n, pl.ds(0, NC - 1)]
        return remote(part, part, s.at[n], r.at[n], mate)

    def send_back(dst, s, r, n):
        others(
            lambda i: remote(px.at[n, i], piece_of(dst, n, chip), s.at[n], r.at[n], at(i)).start()
        )

    def all_back(s, r, n):
        part = px.at[n, pl.ds(0, NC - 1)]
        return remote(part, part, s.at[n], r.at[n], mate)

    def all_home(dst, s, r, n):
        part = dst.at[n, pl.ds(0, (NC - 1) * RS), :]
        return remote(part, part, s.at[n], r.at[n], mate)

    def prefix(recv, dst, s, r, n, reverse):
        head = own0 + n * HG + (chip * RS) // DH
        mine = pl.ds(pl.multiple_of(chip * RS, RS), RS)
        recv[n, chip] = tot[n, mine, :]
        all_in(recv, s, r, n).wait_recv()
        state = jnp.zeros((RS, DH), F32)
        for i in reversed(range(NC)) if reverse else range(NC):
            px[n, i] = state
            state = jnp.exp(dec_all[i, head]) * state + recv[n, i]
        dst[n, mine, :] = px[n, chip]

    def settle(first, homed, recv, dst, n):
        def one(r):
            h = own0 + n * HG + r
            state = homed[n, pl.ds(pl.multiple_of(r * DH, DH), DH), :]
            ahead = jnp.where(first, 1.0, jnp.exp(dec_par[h]))
            dst[h] = ahead * state + jnp.where(first, 0.0, recv[n, r])
            after = jnp.where(first, jnp.exp(dec_own[h]), 1.0)
            pst[n, r] = after * state + jnp.where(first, loc[h], 0.0)

        loop(HG, one)

    dec_copy = remote(dec_own, dec_par, dp_s.at[0], dp_r.at[0], mate)

    def dec_send(i):
        return remote(dec_chip, dec_all.at[chip], da_s.at[0], da_r.at[0], at(i))

    dec_part = dec_all.at[pl.ds(0, NC - 1)]
    dec_done = remote(dec_part, dec_part, da_s.at[0], da_r.at[0], mate)

    loads[0].wait()
    loads[1].wait()
    loop(HG, lambda r: local_states(oth0 + r))
    pl.semaphore_wait(barrier, NC - 1 + 1 + NY - 1)
    dec_copy.start()
    swap(loc, lpr, lp_s, lp_r, 0).start()
    loop(HG, lambda r: local_states(own0 + r))
    dec_copy.wait()
    dec_chip[...] = dec_own[...] + dec_par[...]
    dec_all[chip] = dec_chip[...]
    others(lambda i: dec_send(i).start())
    swap(loc, lpr, lp_s, lp_r, 0).wait()
    scan_total(core == 0, lpr, 0)
    loop(HG, lambda r: local_states(oth0 + HG + r))
    send_out(rx, rx_s, rx_r, 0)
    swap(loc, lpr, lp_s, lp_r, 1).start()
    loop(HG, lambda r: local_states(own0 + HG + r))
    swap(loc, lpr, lp_s, lp_r, 1).wait()
    scan_total(core == 0, lpr, 1)
    send_out(rx, rx_s, rx_r, 1)

    loads[2].wait()

    def intra(h):
        for j in range(NJ):
            qj, vj = tile(q, h, j), tile(v, h, j)
            decay = jnp.exp(jnp.where(lower, cums(h, j) - cum_row(h, j), -jnp.inf))
            weights = (nn(qj, tile(kt, h, j)) * decay).astype(BF16)
            put(att, h, j, nn(weights, vj))
            put(wt, h, j, weights.T)
            put(ga, h, j, qj.T)
            put(kt, h, j, vj.T)

    def spans(n):
        first = (3 * n) // 8
        second = (6 * n) // 8
        return first, second

    cut0, cut1 = spans(H)
    loop(cut0, intra)
    dec_done.wait()
    prefix(rx, pin, rx_s, rx_r, 0, False)
    send_back(pin, pi_s, pi_r, 0)
    loop(cut1 - cut0, lambda r: intra(cut0 + r))
    prefix(rx, pin, rx_s, rx_r, 1, False)
    send_back(pin, pi_s, pi_r, 1)
    loop(H - cut1, lambda r: intra(cut1 + r))
    loads[3].wait()
    acc_s[...] = jnp.zeros_like(acc_s)
    acc_c[...] = jnp.zeros_like(acc_c)

    def inter(h):
        states = [st[h + p] for p in range(PAIR)]
        scales = [gain[:, pl.ds(pl.multiple_of((h + p) * DH, DH), DH)] for p in range(PAIR)]
        for j in range(NJ):
            squares, crosses = None, None
            for p in range(PAIR):
                cum = cums(h + p, j)
                low = states[p].astype(BF16)
                sbf[h + p, j] = low
                mixed = tile(att, h + p, j) + jnp.exp(cum) * nn(tile(q, h + p, j), low)
                put(att, h + p, j, mixed)
                square = mixed * mixed
                cross = tile(g, h + p, j).astype(F32) * scales[p] * mixed
                squares = square if squares is None else squares + square
                crosses = cross if crosses is None else crosses + cross
                if j < NJ - 1:
                    states[p] = jnp.exp(cum[DH - 1:DH, :]) * states[p] + ms[h + p, j]
            acc_s[j * DH:(j + 1) * DH, :] += squares
            acc_c[j * DH:(j + 1) * DH, :] += crosses

    for n in range(2):
        all_home(pin, pi_s, pi_r, n).wait_recv()
        settle(core == 0, pin, lpr, st, n)
        give(st, ps_s, ps_r, n, own0).start()
        loop(HG // PAIR, lambda r: inter(own0 + n * HG + r * PAIR))
    for n in range(2):
        give(st, ps_s, ps_r, n, oth0).wait_recv()
        loop(HG // PAIR, lambda r: inter(oth0 + n * HG + r * PAIR))

    pick = lax.broadcasted_iota(jnp.int32, (8, DH), 0) == 0
    for j in range(NJ):
        a = jnp.sum(acc_s[j * DH:(j + 1) * DH, :].T, axis=0, keepdims=True)
        b = jnp.sum(acc_c[j * DH:(j + 1) * DH, :].T, axis=0, keepdims=True)
        sums[:, j * DH:(j + 1) * DH] = jnp.where(pick, a, b)
    for r in range(1, NY):
        d = lax.rem(y + r, NY)
        remote(sums, hx.at[y], hx_s.at[0], hx_r.at[0], {"head": d}).start()
    hx[y] = sums[...]

    def turn(h):
        for j in range(NJ):
            sbf[h, j] = sbf[h, j].T

    loop(H, turn)
    for n in range(2):
        all_out(rx, rx_s, rx_r, n).wait_send()
        all_back(pi_s, pi_r, n).wait_send()
        give(st, ps_s, ps_r, n, own0).wait_send()
    hx_part = hx.at[pl.ds(0, NY - 1)]
    remote(hx_part, hx_part, hx_s.at[0], hx_r.at[0], mate).wait()
    for j in range(NJ):
        both = hx[0, :, j * DH:(j + 1) * DH]
        for r in range(1, NY):
            both = both + hx[r, :, j * DH:(j + 1) * DH]
        inverse = lax.rsqrt(both[0:1, :] / HD + EPSILON)
        center = both[1:2, :] * inverse / HD
        columns = jnp.where(pick, inverse, center).T
        acc_s[j * DH:(j + 1) * DH, :] = jnp.broadcast_to(columns[:, 0:1], (DH, DH))
        acc_c[j * DH:(j + 1) * DH, :] = jnp.broadcast_to(columns[:, 1:2], (DH, DH))

    def normalize(h):
        scale = gain[:, pl.ds(pl.multiple_of(h * DH, DH), DH)]
        gain_part = jnp.zeros((8, DH), F32)
        for j in range(NJ):
            inverse = acc_s[j * DH:(j + 1) * DH, :]
            normed = tile(att, h, j) * inverse
            grad = tile(g, h, j).astype(F32)
            put(g, h, j, (normed * scale).astype(BF16))
            gain_part = gain_part + jnp.sum((grad * normed).reshape(DH // 8, 8, DH), axis=0)
            center = acc_c[j * DH:(j + 1) * DH, :]
            low = (inverse * (grad * scale - normed * center)).astype(BF16)
            lifted = tile(ga, h, j).astype(F32) * jnp.exp(cum_row(h, j))
            ms[h, j] = nn(lifted.astype(BF16), low)
            put(ga, h, j, low)
        ggp[h] = gain_part
        state = ms[h, NJ - 1]
        for j in range(NJ - 2, -1, -1):
            end = cb[h, j * DH + DH - 1:j * DH + DH, :]
            state = jnp.exp(end) * state + ms[h, j]
        loc[h] = state

    for n in range(2):
        loop(HG, lambda r: normalize(oth0 + n * HG + r))
        swap(loc, lpr, glp_s, glp_r, n).start()
        loop(HG, lambda r: normalize(own0 + n * HG + r))
        swap(loc, lpr, glp_s, glp_r, n).wait()
        scan_total(core == 1, lpr, n)
        send_out(rx, grx_s, grx_r, n)

    gain_copy = remote(ggp, ggpr, gp_s.at[0], gp_r.at[0], mate)
    gain_copy.start()

    def intra_grads(h):
        for j in range(NJ):
            gj = tile(ga, h, j)
            cum = cums(h, j)
            decay = jnp.exp(jnp.where(lower, cum - cum_row(h, j), -jnp.inf))
            gw = (nn(gj, tile(kt, h, j)) * decay).astype(BF16)
            gq = nn(gw, tile(k, h, j)) + jnp.exp(cum) * nn(gj, sbf[h, j])
            put(gvi, h, j, nn(tile(wt, h, j), gj))
            put(att, h, j, nn(gw.T, tile(q, h, j)))
            put(q, h, j, gq.astype(BF16))

    loop(cut0, intra_grads)
    gain_copy.wait()
    ggc[...] = ggp[...] + ggpr[...]
    ggrx[chip] = ggc[chip]
    prefix(rx, pin, grx_s, grx_r, 0, True)
    send_back(pin, gpi_s, gpi_r, 0)
    others(lambda i: remote(ggc.at[i], ggrx.at[chip], gr_s.at[0], gr_r.at[0], at(i)).start())
    loop(cut1 - cut0, lambda r: intra_grads(cut0 + r))
    prefix(rx, pin, grx_s, grx_r, 1, True)
    send_back(pin, gpi_s, gpi_r, 1)
    gr_part = ggrx.at[pl.ds(0, NC - 1)]
    remote(gr_part, gr_part, gr_s.at[0], gr_r.at[0], mate).wait()
    part = ggrx[0]
    for i in range(1, NC):
        part = part + ggrx[i]
    ggsum[...] = part
    ggall[chip] = part
    others(lambda i: remote(ggsum, ggall.at[chip], ga_s.at[0], ga_r.at[0], at(i)).start())
    loop(H - cut1, lambda r: intra_grads(cut1 + r))

    def later_states(h):
        state = st[h]
        for j in range(NJ - 1, -1, -1):
            sbf[h, j] = state.astype(BF16)
            if j > 0:
                state = jnp.exp(cb[h, j * DH + DH - 1:j * DH + DH, :]) * state + ms[h, j]

    def own_grads(h):
        later_states(h)
        inter_grads(sizes, h, h, k, v, cb, sbf, att, gvi, k, v)

    for n in range(2):
        all_home(pin, gpi_s, gpi_r, n).wait_recv()
        settle(core == 1, pin, lpr, st, n)
        give(st, gps_s, gps_r, n, own0).start()
        loop(HG, lambda r: own_grads(own0 + n * HG + r))
    for n in range(2):
        give(st, gps_s, gps_r, n, oth0).wait_recv()
        loop(HG, lambda r: later_states(oth0 + n * HG + r))

    gg_part = ggall.at[pl.ds(0, NC - 1)]
    remote(gg_part, gg_part, ga_s.at[0], ga_r.at[0], mate).wait()
    for h in range(H):
        gg_out[h:h + 1, :] = jnp.sum(ggall[h], axis=0, keepdims=True)
    for n in range(2):
        all_out(rx, grx_s, grx_r, n).wait_send()
        all_back(gpi_s, gpi_r, n).wait_send()
        give(st, gps_s, gps_r, n, own0).wait_send()


def on_device(sizes, queries, key_rows, value_rows, log_decay, norm_gain, grad_out):
    T, H, NC, NY = sizes
    W = H * DH
    NJ = T // DH
    HH = H // 2
    HG = HH // 2
    RS = HG * DH // NC
    V = pltpu.VMEM
    D = pltpu.SemaphoreType.DMA
    rows = V((2, HG * DH, DH), F32)
    slots = V((2, NC, RS, DH), F32)
    heads = V((2, HG, DH, DH), F32)
    states = V((H, DH, DH), F32)
    scratch = [
        V((H, 1, T), F32), V((H, NJ, DH, DH), F32), V((T, W), BF16), V((T, W), BF16),
        V((T, W), BF16),
        V((T, DH), F32), V((T, DH), F32),
        V((8, T), F32), V((NY, 8, T), F32),
        V((H, 1, DH), F32), V((H, 1, DH), F32), V((H, 1, DH), F32), V((NC, H, 1, DH), F32),
        states, rows, slots, heads, heads, slots, rows, states,
        V((H, 8, DH), F32), V((H, 8, DH), F32), V((H, 8, DH), F32), V((NC, 8, DH), F32),
        V((8, DH), F32), V((NC, 8, DH), F32),
        D((4,)), *[D((1,))] * 6, *[D((2,))] * 16, *[D((1,))] * 6,
    ]
    anywhere = pl.BlockSpec(memory_space=pl.ANY)
    local = pl.BlockSpec(memory_space=V)
    held = (
        V((T, W), BF16), V((T, W), BF16), V((T, W), BF16), V((T, W), BF16),
        V((H, T, DH), F32), V((H, NJ, DH, DH), BF16), V((T, W), F32), V((T, W), F32),
        V((H, DH), F32),
    )
    parts = pl.pallas_call(
        functools.partial(kernel, sizes),
        out_shape=held,
        in_specs=[anywhere, anywhere, anywhere, local, local, anywhere],
        out_specs=(local,) * len(held),
        scratch_shapes=scratch,
        compiler_params=pltpu.CompilerParams(
            collective_id=0, has_side_effects=True, vmem_limit_bytes=23 << 20
        ),
    )(queries, key_rows, value_rows, log_decay, norm_gain.reshape(1, W), grad_out)
    parts = [pltpu.with_memory_space_constraint(x, V) for x in parts]
    big = jax.ShapeDtypeStruct((T, W), BF16)
    *grads, gain_grad = pl.pallas_call(
        functools.partial(finish, sizes),
        out_shape=(big, big, big, big, jax.ShapeDtypeStruct((H, DH), F32)),
        in_specs=[local] * len(held),
        out_specs=(anywhere, anywhere, anywhere, anywhere, local),
        scratch_shapes=[
            V((T, W // 2), BF16), V((T, W // 2), BF16), D((4,)), D((2, HH)),
        ],
        compiler_params=pltpu.CompilerParams(vmem_limit_bytes=5 << 20),
    )(*parts)
    return (*grads, gain_grad.reshape(W))


def solution(mesh):
    def whole(queries, key_rows, value_rows, log_decay, norm_gain, grad_out):
        seq, head = mesh.shape["seq"], mesh.shape["head"]
        sizes = (queries.shape[0] // seq, queries.shape[1] // DH // head, seq // 2, head)
        rows = P("seq", "head")
        return jax.shard_map(
            functools.partial(on_device, sizes),
            mesh=mesh,
            in_specs=(rows, rows, rows, P("head", "seq"), P("head"), rows),
            out_specs=(rows, rows, rows, rows, P("head")),
            check_vma=False,
        )(queries, key_rows, value_rows, log_decay, norm_gain, grad_out)

    return whole
```

```python
import functools

import jax
import jax.numpy as jnp
from jax import lax
from jax.experimental import pallas as pl
from jax.experimental.pallas import tpu as pltpu
from jax.sharding import PartitionSpec as P

DH = 128
EPSILON = 1e-06
F32 = jnp.float32
BF16 = jnp.bfloat16
MESH = pl.DeviceIdType.MESH
HIGHEST = lax.Precision.HIGHEST


def groups_of(heads):
    return 4 if heads % 8 == 0 else 2


def nn(a, b):
    return lax.dot_general(a, b, (((1,), (0,)), ((), ())), preferred_element_type=F32)


def nt(a, b):
    return lax.dot_general(a, b, (((1,), (1,)), ((), ())), preferred_element_type=F32)


def tn(a, b):
    return lax.dot_general(a, b, (((0,), (0,)), ((), ())), preferred_element_type=F32)


def exact_nt(a, b):
    return lax.dot_general(
        a, b, (((1,), (1,)), ((), ())), preferred_element_type=F32, precision=HIGHEST
    )


def tile(ref, h, j):
    return ref[j * DH:(j + 1) * DH, pl.ds(pl.multiple_of(h * DH, DH), DH)]


def put(ref, h, j, value):
    ref[j * DH:(j + 1) * DH, pl.ds(pl.multiple_of(h * DH, DH), DH)] = value


def inter_grads(sizes, h, to, k, v, cb, sbf, att, gvi, gk, gv):
    for j in range(sizes[0] // DH):
        cum = cb[h, j * DH:(j + 1) * DH, :]
        low = sbf[h, j]
        tail = jnp.exp(cum[DH - 1:DH, :] - cum)
        kj, vj = tile(k, h, j), tile(v, h, j)
        put(gk, to, j, (tile(att, h, j) + tail * nn(vj, low.T)).astype(BF16))
        put(gv, to, j, (tile(gvi, h, j) + tail * nn(kj, low)).astype(BF16))


def finish(
    sizes,
    q, k, v, g, cb, sbf, att, gvi, gg,
    out_hbm, gq_hbm, gk_hbm, gv_hbm, gg_out,
    gk, gv, sem, head_sem,
):
    HH = sizes[1] // 2
    HW = HH * DH
    core = lax.axis_index("seq") % 2
    own = pl.ds(pl.multiple_of(core * HW, HW), HW)
    copies = [
        pltpu.make_async_copy(src, dst, sem.at[n])
        for n, (src, dst) in enumerate((
            (g, out_hbm), (q, gq_hbm),
            (k.at[:, own], gk_hbm.at[:, own]), (v.at[:, own], gv_hbm.at[:, own]),
        ))
    ]
    for c in copies:
        c.start()
    gg_out[...] = gg[...]

    def stores(r):
        src = pl.ds(pl.multiple_of(r * DH, DH), DH)
        dst = pl.ds(pl.multiple_of(((1 - core) * HH + r) * DH, DH), DH)
        return [
            pltpu.make_async_copy(a.at[:, src], b.at[:, dst], head_sem.at[n, r])
            for n, (a, b) in enumerate(((gk, gk_hbm), (gv, gv_hbm)))
        ]

    def one(r, carry):
        inter_grads(sizes, (1 - core) * HH + r, r, k, v, cb, sbf, att, gvi, gk, gv)
        for c in stores(r):
            c.start()
        return carry

    lax.fori_loop(0, HH, one, 0)
    for r in range(HH):
        for c in stores(r):
            c.wait()
    for c in copies:
        c.wait()


def kernel(
    sizes,
    q_in, k_in, v_in, ld, gain, g_in,
    q, k, v, g, cb, sbf, att, gvi, gg_out,
    rc, ms, ga, kt, wt,
    acc_s, acc_c, sums, hx,
    dec_own, dec_par, dec_chip, dec_all,
    loc, tot, px, pst, lpr, rx, pin, st,
    ggp, ggpr, ggc, ggrx, ggsum, ggall,
    in_sem, dp_s, dp_r, da_s, da_r, hx_s, hx_r,
    lp_s, lp_r, rx_s, rx_r, pi_s, pi_r, ps_s, ps_r,
    glp_s, glp_r, grx_s, grx_r, gpi_s, gpi_r, gps_s, gps_r,
    gp_s, gp_r, gr_s, gr_r, ga_s, ga_r,
):
    T, H, NC, NY = sizes
    NJ = T // DH
    HH = H // 2
    G = groups_of(HH)
    HG = HH // G
    RS = HG * DH // NC
    HD = NY * H * DH
    PAIR = 2 if HG % 2 == 0 else 1
    U = H // PAIR
    me = lax.axis_index("seq")
    y = lax.axis_index("head")
    chip = me // 2
    core = me % 2
    mate = {"seq": chip * 2 + (1 - core)}
    own0 = core * HH
    oth0 = (1 - core) * HH

    def at(i):
        return {"seq": i * 2 + core}

    def remote(src, dst, s, r, dev):
        return pltpu.make_async_remote_copy(
            src_ref=src, dst_ref=dst, send_sem=s, recv_sem=r, device_id=dev, device_id_type=MESH
        )

    def loop(n, body):
        lax.fori_loop(0, n, lambda i, c: (body(i), c)[1], 0)

    def span(first, n, body):
        lax.fori_loop(first, n, lambda i, c: (body(i), c)[1], 0)

    def heads(base, body):
        def one(r):
            for p in range(PAIR):
                body(base + r * PAIR + p)

        loop(HG // PAIR, one)

    def units(first, n, body):
        def one(r):
            for p in range(PAIR):
                body((first + r) * PAIR + p)

        loop(n, one)

    def others(body):
        lax.fori_loop(1, NC, lambda r, c: (body(lax.rem(chip + r, NC)), c)[1], 0)

    loads = [
        pltpu.make_async_copy(src, dst, in_sem.at[n])
        for n, (src, dst) in enumerate(((k_in, k), (v_in, v), (q_in, q), (g_in, g)))
    ]
    loads[0].start()
    loads[1].start()

    barrier = pltpu.get_barrier_semaphore()
    others(
        lambda i: pl.semaphore_signal(barrier, inc=1, device_id=at(i), device_id_type=MESH)
    )
    pl.semaphore_signal(barrier, inc=1, device_id=mate, device_id_type=MESH)
    for r in range(1, NY):
        pl.semaphore_signal(
            barrier, inc=1, device_id={"head": lax.rem(y + r, NY)}, device_id_type=MESH
        )

    row_i = lax.broadcasted_iota(jnp.int32, (DH, DH), 0)
    col_i = lax.broadcasted_iota(jnp.int32, (DH, DH), 1)
    lower = row_i >= col_i
    tri = jnp.where(lower, 1.0, 0.0).astype(F32)

    total = jnp.zeros((H, 1), F32)
    for j in range(NJ):
        piece = ld[:, j * DH:(j + 1) * DH]
        rows = exact_nt(piece, tri)
        columns = exact_nt(tri, piece)
        for h in range(H):
            rc[h, :, j * DH:(j + 1) * DH] = rows[h:h + 1, :]
            cb[h, j * DH:(j + 1) * DH, :] = jnp.broadcast_to(columns[:, h:h + 1], (DH, DH))
        total = total + rows[:, DH - 1:DH]
    dec_own[...] = jnp.broadcast_to(total, (H, DH)).reshape(H, 1, DH)
    loads[2].start()
    loads[3].start()

    def cums(h, j):
        return cb[h, j * DH:(j + 1) * DH, :]

    def cum_row(h, j):
        return rc[h, :, j * DH:(j + 1) * DH]

    def local_states(h):
        state = None
        for j in range(NJ):
            row = cum_row(h, j)
            end = row[:, DH - 1:DH]
            flipped = tile(k, h, j).T
            put(kt, h, j, flipped)
            scaled = (flipped.astype(F32) * jnp.exp(end - row)).astype(BF16)
            part = nn(scaled, tile(v, h, j))
            ms[h, j] = part
            last = jnp.exp(cb[h, j * DH + DH - 1:j * DH + DH, :])
            state = part if state is None else last * state + part
        loc[h] = state

    def group(ref, base, n):
        return ref.at[pl.ds(base + n * HG, HG)]

    def swap(src, recv, s, r, n):
        return remote(group(src, oth0, n), recv.at[n], s.at[n], r.at[n], mate)

    def give(dst, s, r, n, base):
        return remote(pst.at[n], group(dst, base, n), s.at[n], r.at[n], mate)

    def scan_total(first, recv, n):
        def one(r):
            h = own0 + n * HG + r
            mine = jnp.where(first, jnp.exp(dec_par[h]), 1.0)
            theirs = jnp.where(first, 1.0, jnp.exp(dec_own[h]))
            tot[n, pl.ds(pl.multiple_of(r * DH, DH), DH), :] = mine * loc[h] + theirs * recv[n, r]

        loop(HG, one)

    side = 4 if NC == 16 else 2
    steps = [(a, b) for a in range(side) for b in range(side) if a + b > 0]
    steps.sort(key=lambda ab: -sum(min(d, side - d) for d in ab))

    def farthest(body):
        for a, b in steps:
            body(lax.rem(chip // side + a, side) * side + lax.rem(chip % side + b, side))

    def piece_of(ref, n, i):
        return ref.at[n, pl.ds(pl.multiple_of(i * RS, RS), RS), :]

    def send_out(recv, s, r, n):
        farthest(
            lambda i: remote(piece_of(tot, n, i), recv.at[n, chip], s.at[n], r.at[n], at(i)).start()
        )

    def all_out(recv, s, r, n):
        return remote(
            tot.at[n, pl.ds(0, (NC - 1) * RS), :], tot.at[n, pl.ds(0, (NC - 1) * RS), :],
            s.at[n], r.at[n], mate,
        )

    def all_in(recv, s, r, n):
        part = recv.at[n, pl.ds(0, NC - 1)]
        return remote(part, part, s.at[n], r.at[n], mate)

    def send_back(dst, s, r, n):
        farthest(
            lambda i: remote(px.at[n, i], piece_of(dst, n, chip), s.at[n], r.at[n], at(i)).start()
        )

    def all_back(s, r, n):
        part = px.at[n, pl.ds(0, NC - 1)]
        return remote(part, part, s.at[n], r.at[n], mate)

    def all_home(dst, s, r, n):
        part = dst.at[n, pl.ds(0, (NC - 1) * RS), :]
        return remote(part, part, s.at[n], r.at[n], mate)

    def prefix(recv, dst, s, r, n, reverse):
        head = own0 + n * HG + (chip * RS) // DH
        mine = pl.ds(pl.multiple_of(chip * RS, RS), RS)
        recv[n, chip] = tot[n, mine, :]
        all_in(recv, s, r, n).wait_recv()
        state = jnp.zeros((RS, DH), F32)
        for i in reversed(range(NC)) if reverse else range(NC):
            px[n, i] = state
            state = jnp.exp(dec_all[i, head]) * state + recv[n, i]
        dst[n, mine, :] = px[n, chip]

    def settle(first, homed, recv, dst, n):
        def one(r):
            h = own0 + n * HG + r
            state = homed[n, pl.ds(pl.multiple_of(r * DH, DH), DH), :]
            ahead = jnp.where(first, 1.0, jnp.exp(dec_par[h]))
            dst[h] = ahead * state + jnp.where(first, 0.0, recv[n, r])
            after = jnp.where(first, jnp.exp(dec_own[h]), 1.0)
            pst[n, r] = after * state + jnp.where(first, loc[h], 0.0)

        loop(HG, one)

    dec_copy = remote(dec_own, dec_par, dp_s.at[0], dp_r.at[0], mate)

    def dec_send(i):
        return remote(dec_chip, dec_all.at[chip], da_s.at[0], da_r.at[0], at(i))

    dec_part = dec_all.at[pl.ds(0, NC - 1)]
    dec_done = remote(dec_part, dec_part, da_s.at[0], da_r.at[0], mate)

    loads[0].wait()
    loads[1].wait()
    heads(oth0, local_states)
    pl.semaphore_wait(barrier, NC - 1 + 1 + NY - 1)
    dec_copy.start()
    swap(loc, lpr, lp_s, lp_r, 0).start()

    def for_mate(n):
        heads(oth0 + n * HG, local_states)
        swap(loc, lpr, lp_s, lp_r, n).start()

    span(1, G, for_mate)
    dec_copy.wait()
    dec_chip[...] = dec_own[...] + dec_par[...]
    dec_all[chip] = dec_chip[...]
    others(lambda i: dec_send(i).start())

    def for_own(n):
        heads(own0 + n * HG, local_states)
        swap(loc, lpr, lp_s, lp_r, n).wait()
        scan_total(core == 0, lpr, n)
        send_out(rx, rx_s, rx_r, n)

    loop(G, for_own)

    loads[2].wait()

    def intra(h):
        for j in range(NJ):
            qj, vj = tile(q, h, j), tile(v, h, j)
            decay = jnp.exp(jnp.where(lower, cums(h, j) - cum_row(h, j), -jnp.inf))
            weights = (nn(qj, tile(kt, h, j)) * decay).astype(BF16)
            put(att, h, j, nn(weights, vj))
            put(wt, h, j, weights.T)
            lifted = qj.T.astype(F32) * jnp.exp(cum_row(h, j))
            put(ga, h, j, lifted.astype(BF16))
            put(kt, h, j, vj.T)

    ahead = U // 4
    units(0, ahead, intra)
    dec_done.wait()

    def forward(n):
        prefix(rx, pin, rx_s, rx_r, n, False)
        send_back(pin, pi_s, pi_r, n)
        units(ahead + n, 1, intra)

    loop(G, forward)
    units(ahead + G, U - ahead - G, intra)
    loads[3].wait()
    acc_s[...] = jnp.zeros_like(acc_s)
    acc_c[...] = jnp.zeros_like(acc_c)

    def inter(h):
        states = [st[h + p] for p in range(PAIR)]
        scales = [gain[:, pl.ds(pl.multiple_of((h + p) * DH, DH), DH)] for p in range(PAIR)]
        for j in range(NJ):
            squares, crosses = None, None
            for p in range(PAIR):
                cum = cums(h + p, j)
                low = states[p].astype(BF16)
                sbf[h + p, j] = low
                mixed = tile(att, h + p, j) + jnp.exp(cum) * nn(tile(q, h + p, j), low)
                put(att, h + p, j, mixed)
                square = mixed * mixed
                cross = tile(g, h + p, j).astype(F32) * scales[p] * mixed
                squares = square if squares is None else squares + square
                crosses = cross if crosses is None else crosses + cross
                if j < NJ - 1:
                    states[p] = jnp.exp(cum[DH - 1:DH, :]) * states[p] + ms[h + p, j]
            acc_s[j * DH:(j + 1) * DH, :] += squares
            acc_c[j * DH:(j + 1) * DH, :] += crosses

    def mine(n):
        all_home(pin, pi_s, pi_r, n).wait_recv()
        settle(core == 0, pin, lpr, st, n)
        give(st, ps_s, ps_r, n, own0).start()
        loop(HG // PAIR, lambda r: inter(own0 + n * HG + r * PAIR))

    def theirs(n):
        give(st, ps_s, ps_r, n, oth0).wait_recv()
        loop(HG // PAIR, lambda r: inter(oth0 + n * HG + r * PAIR))

    loop(G, mine)
    loop(G, theirs)

    pick = lax.broadcasted_iota(jnp.int32, (8, DH), 0) == 0
    for j in range(NJ):
        a = jnp.sum(acc_s[j * DH:(j + 1) * DH, :].T, axis=0, keepdims=True)
        b = jnp.sum(acc_c[j * DH:(j + 1) * DH, :].T, axis=0, keepdims=True)
        sums[:, j * DH:(j + 1) * DH] = jnp.where(pick, a, b)
    for r in range(1, NY):
        d = lax.rem(y + r, NY)
        remote(sums, hx.at[y], hx_s.at[0], hx_r.at[0], {"head": d}).start()
    hx[y] = sums[...]

    def turn(h):
        for j in range(NJ):
            sbf[h, j] = sbf[h, j].T

    units(0, U, turn)

    def sent(n):
        all_out(rx, rx_s, rx_r, n).wait_send()
        all_back(pi_s, pi_r, n).wait_send()
        give(st, ps_s, ps_r, n, own0).wait_send()

    loop(G, sent)
    hx_part = hx.at[pl.ds(0, NY - 1)]
    remote(hx_part, hx_part, hx_s.at[0], hx_r.at[0], mate).wait()
    for j in range(NJ):
        both = hx[0, :, j * DH:(j + 1) * DH]
        for r in range(1, NY):
            both = both + hx[r, :, j * DH:(j + 1) * DH]
        inverse = lax.rsqrt(both[0:1, :] / HD + EPSILON)
        center = both[1:2, :] * inverse / HD
        columns = jnp.where(pick, inverse, center).T
        acc_s[j * DH:(j + 1) * DH, :] = jnp.broadcast_to(columns[:, 0:1], (DH, DH))
        acc_c[j * DH:(j + 1) * DH, :] = jnp.broadcast_to(columns[:, 1:2], (DH, DH))

    def normalize(h):
        scale = gain[:, pl.ds(pl.multiple_of(h * DH, DH), DH)]
        gain_part = jnp.zeros((8, DH), F32)
        for j in range(NJ):
            inverse = acc_s[j * DH:(j + 1) * DH, :]
            normed = tile(att, h, j) * inverse
            grad = tile(g, h, j).astype(F32)
            put(g, h, j, (normed * scale).astype(BF16))
            gain_part = gain_part + jnp.sum((grad * normed).reshape(DH // 8, 8, DH), axis=0)
            center = acc_c[j * DH:(j + 1) * DH, :]
            low = (inverse * (grad * scale - normed * center)).astype(BF16)
            ms[h, j] = nn(tile(ga, h, j), low)
            put(ga, h, j, low)
        ggp[h] = gain_part
        state = ms[h, NJ - 1]
        for j in range(NJ - 2, -1, -1):
            end = cb[h, j * DH + DH - 1:j * DH + DH, :]
            state = jnp.exp(end) * state + ms[h, j]
        loc[h] = state

    def grads_mate(n):
        heads(oth0 + n * HG, normalize)
        swap(loc, lpr, glp_s, glp_r, n).start()

    def grads_own(n):
        heads(own0 + n * HG, normalize)
        swap(loc, lpr, glp_s, glp_r, n).wait()
        scan_total(core == 1, lpr, n)
        send_out(rx, grx_s, grx_r, n)

    loop(G, grads_mate)
    loop(G, grads_own)

    gain_copy = remote(ggp, ggpr, gp_s.at[0], gp_r.at[0], mate)
    gain_copy.start()

    def intra_grads(h):
        for j in range(NJ):
            gj = tile(ga, h, j)
            cum = cums(h, j)
            decay = jnp.exp(jnp.where(lower, cum - cum_row(h, j), -jnp.inf))
            gw = (nn(gj, tile(kt, h, j)) * decay).astype(BF16)
            grown = (gj.astype(F32) * jnp.exp(cum)).astype(BF16)
            gq = nn(gw, tile(k, h, j)) + nn(grown, sbf[h, j])
            put(gvi, h, j, nn(tile(wt, h, j), gj))
            put(att, h, j, nn(gw.T, tile(q, h, j)))
            put(q, h, j, gq.astype(BF16))

    soon = U // 8
    units(0, soon, intra_grads)
    gain_copy.wait()
    ggc[...] = ggp[...] + ggpr[...]
    ggrx[chip] = ggc[chip]
    others(lambda i: remote(ggc.at[i], ggrx.at[chip], gr_s.at[0], gr_r.at[0], at(i)).start())

    def backward(n):
        prefix(rx, pin, grx_s, grx_r, n, True)
        send_back(pin, gpi_s, gpi_r, n)
        units(soon + n, 1, intra_grads)

    loop(G, backward)
    gr_part = ggrx.at[pl.ds(0, NC - 1)]
    remote(gr_part, gr_part, gr_s.at[0], gr_r.at[0], mate).wait()
    part = ggrx[0]
    for i in range(1, NC):
        part = part + ggrx[i]
    ggsum[...] = part
    ggall[chip] = part
    others(lambda i: remote(ggsum, ggall.at[chip], ga_s.at[0], ga_r.at[0], at(i)).start())
    units(soon + G, U - soon - G, intra_grads)

    def later_states(h):
        state = st[h]
        for j in range(NJ - 1, -1, -1):
            sbf[h, j] = state.astype(BF16)
            if j > 0:
                state = jnp.exp(cb[h, j * DH + DH - 1:j * DH + DH, :]) * state + ms[h, j]

    def own_grads(h):
        later_states(h)
        inter_grads(sizes, h, h, k, v, cb, sbf, att, gvi, k, v)

    def last_mine(n):
        all_home(pin, gpi_s, gpi_r, n).wait_recv()
        settle(core == 1, pin, lpr, st, n)
        give(st, gps_s, gps_r, n, own0).start()
        heads(own0 + n * HG, own_grads)

    def last_theirs(n):
        give(st, gps_s, gps_r, n, oth0).wait_recv()
        heads(oth0 + n * HG, later_states)

    loop(G, last_mine)
    loop(G, last_theirs)

    gg_part = ggall.at[pl.ds(0, NC - 1)]
    remote(gg_part, gg_part, ga_s.at[0], ga_r.at[0], mate).wait()
    for h in range(H):
        gg_out[h:h + 1, :] = jnp.sum(ggall[h], axis=0, keepdims=True)
    def done(n):
        all_out(rx, grx_s, grx_r, n).wait_send()
        all_back(gpi_s, gpi_r, n).wait_send()
        give(st, gps_s, gps_r, n, own0).wait_send()

    loop(G, done)


def on_device(sizes, queries, key_rows, value_rows, log_decay, norm_gain, grad_out):
    T, H, NC, NY = sizes
    W = H * DH
    NJ = T // DH
    HH = H // 2
    G = groups_of(HH)
    HG = HH // G
    RS = HG * DH // NC
    V = pltpu.VMEM
    D = pltpu.SemaphoreType.DMA
    rows = V((G, HG * DH, DH), F32)
    slots = V((G, NC, RS, DH), F32)
    heads = V((G, HG, DH, DH), F32)
    states = V((H, DH, DH), F32)
    scratch = [
        V((H, 1, T), F32), V((H, NJ, DH, DH), F32), V((T, W), BF16), V((T, W), BF16),
        V((T, W), BF16),
        V((T, DH), F32), V((T, DH), F32),
        V((8, T), F32), V((NY, 8, T), F32),
        V((H, 1, DH), F32), V((H, 1, DH), F32), V((H, 1, DH), F32), V((NC, H, 1, DH), F32),
        states, rows, slots, heads, heads, slots, rows, states,
        V((H, 8, DH), F32), V((H, 8, DH), F32), V((H, 8, DH), F32), V((NC, 8, DH), F32),
        V((8, DH), F32), V((NC, 8, DH), F32),
        D((4,)), *[D((1,))] * 6, *[D((G,))] * 16, *[D((1,))] * 6,
    ]
    anywhere = pl.BlockSpec(memory_space=pl.ANY)
    local = pl.BlockSpec(memory_space=V)
    held = (
        V((T, W), BF16), V((T, W), BF16), V((T, W), BF16), V((T, W), BF16),
        V((H, T, DH), F32), V((H, NJ, DH, DH), BF16), V((T, W), F32), V((T, W), F32),
        V((H, DH), F32),
    )
    parts = pl.pallas_call(
        functools.partial(kernel, sizes),
        out_shape=held,
        in_specs=[anywhere, anywhere, anywhere, local, local, anywhere],
        out_specs=(local,) * len(held),
        scratch_shapes=scratch,
        compiler_params=pltpu.CompilerParams(
            collective_id=0, has_side_effects=True, vmem_limit_bytes=23 << 20
        ),
    )(queries, key_rows, value_rows, log_decay, norm_gain.reshape(1, W), grad_out)
    parts = [pltpu.with_memory_space_constraint(x, V) for x in parts]
    big = jax.ShapeDtypeStruct((T, W), BF16)
    *grads, gain_grad = pl.pallas_call(
        functools.partial(finish, sizes),
        out_shape=(big, big, big, big, jax.ShapeDtypeStruct((H, DH), F32)),
        in_specs=[local] * len(held),
        out_specs=(anywhere, anywhere, anywhere, anywhere, local),
        scratch_shapes=[
            V((T, W // 2), BF16), V((T, W // 2), BF16), D((4,)), D((2, HH)),
        ],
        compiler_params=pltpu.CompilerParams(vmem_limit_bytes=5 << 20),
    )(*parts)
    return (*grads, gain_grad.reshape(W))


def solution(mesh):
    def whole(queries, key_rows, value_rows, log_decay, norm_gain, grad_out):
        seq, head = mesh.shape["seq"], mesh.shape["head"]
        sizes = (queries.shape[0] // seq, queries.shape[1] // DH // head, seq // 2, head)
        rows = P("seq", "head")
        return jax.shard_map(
            functools.partial(on_device, sizes),
            mesh=mesh,
            in_specs=(rows, rows, rows, P("head", "seq"), P("head"), rows),
            out_specs=(rows, rows, rows, rows, P("head")),
            check_vma=False,
        )(queries, key_rows, value_rows, log_decay, norm_gain, grad_out)

    return whole
```

```python
import functools

import jax
import jax.numpy as jnp
from jax import lax
from jax.experimental import pallas as pl
from jax.experimental.pallas import tpu as pltpu
from jax.sharding import PartitionSpec as P

DH = 128
EPSILON = 1e-06
F32 = jnp.float32
BF16 = jnp.bfloat16
MESH = pl.DeviceIdType.MESH
HIGHEST = lax.Precision.HIGHEST


def groups_of(heads):
    return 4 if heads % 8 == 0 else 2


def nn(a, b):
    return lax.dot_general(a, b, (((1,), (0,)), ((), ())), preferred_element_type=F32)


def nt(a, b):
    return lax.dot_general(a, b, (((1,), (1,)), ((), ())), preferred_element_type=F32)


def tn(a, b):
    return lax.dot_general(a, b, (((0,), (0,)), ((), ())), preferred_element_type=F32)


def exact_nt(a, b):
    return lax.dot_general(
        a, b, (((1,), (1,)), ((), ())), preferred_element_type=F32, precision=HIGHEST
    )


def tile(ref, h, j):
    return ref[j * DH:(j + 1) * DH, pl.ds(pl.multiple_of(h * DH, DH), DH)]


def put(ref, h, j, value):
    ref[j * DH:(j + 1) * DH, pl.ds(pl.multiple_of(h * DH, DH), DH)] = value


def inter_grads(sizes, h, k, v, cb, sbf, att, gvi, gk, gv):
    for j in range(sizes[0] // DH):
        cum = cb[h, j * DH:(j + 1) * DH, :]
        low = sbf[h, j]
        tail = jnp.exp(cum[DH - 1:DH, :] - cum)
        kj, vj = tile(k, h, j), tile(v, h, j)
        put(gk, h, j, (tile(att, h, j) + tail * nn(vj, low.T)).astype(BF16))
        put(gv, h, j, (tile(gvi, h, j) + tail * nn(kj, low)).astype(BF16))


def finish(
    sizes,
    q, k, v, g, cb, sbf, att, gvi, gg,
    out_hbm, gq_hbm, gk_hbm, gv_hbm, gg_out,
    gk, gv, sem, head_sem,
):
    H = sizes[1]
    copies = [
        pltpu.make_async_copy(src, dst, sem.at[n])
        for n, (src, dst) in enumerate(((g, out_hbm), (q, gq_hbm)))
    ]
    for c in copies:
        c.start()
    gg_out[...] = gg[...]

    def stores(h):
        columns = pl.ds(pl.multiple_of(h * DH, DH), DH)
        return [
            pltpu.make_async_copy(a.at[:, columns], b.at[:, columns], head_sem.at[n, h])
            for n, (a, b) in enumerate(((gk, gk_hbm), (gv, gv_hbm)))
        ]

    def one(h, carry):
        inter_grads(sizes, h, k, v, cb, sbf, att, gvi, gk, gv)
        for c in stores(h):
            c.start()
        return carry

    def ended(h, carry):
        for c in stores(h):
            c.wait()
        return carry

    lax.fori_loop(0, H, one, 0)
    lax.fori_loop(0, H, ended, 0)
    for c in copies:
        c.wait()


def kernel(
    sizes,
    q_in, k_in, v_in, ld, gain, g_in,
    q, k, v, g, cb, sbf, att, gvi, gg_out,
    rc, ms, ga, kt, wt,
    acc_s, acc_c, sums, hx,
    dec_own, dec_par, dec_chip, dec_all,
    loc, tot, px, pst, lpr, rx, pin, st,
    ggp, ggpr, ggc, ggrx, ggsum, ggall,
    in_sem, dp_s, dp_r, da_s, da_r, hx_s, hx_r,
    lp_s, lp_r, rx_s, rx_r, pi_s, pi_r, ps_s, ps_r,
    glp_s, glp_r, grx_s, grx_r, gpi_s, gpi_r, gps_s, gps_r,
    gp_s, gp_r, gr_s, gr_r, ga_s, ga_r,
):
    T, H, NC, NY = sizes
    NJ = T // DH
    HH = H // 2
    G = groups_of(HH)
    HG = HH // G
    RS = HG * DH // NC
    HD = NY * H * DH
    PAIR = 2 if HG % 2 == 0 else 1
    U = H // PAIR
    me = lax.axis_index("seq")
    y = lax.axis_index("head")
    chip = me // 2
    core = me % 2
    mate = {"seq": chip * 2 + (1 - core)}
    own0 = core * HH
    oth0 = (1 - core) * HH

    def at(i):
        return {"seq": i * 2 + core}

    def remote(src, dst, s, r, dev):
        return pltpu.make_async_remote_copy(
            src_ref=src, dst_ref=dst, send_sem=s, recv_sem=r, device_id=dev, device_id_type=MESH
        )

    def loop(n, body):
        lax.fori_loop(0, n, lambda i, c: (body(i), c)[1], 0)

    def span(first, n, body):
        lax.fori_loop(first, n, lambda i, c: (body(i), c)[1], 0)

    def heads(base, body):
        def one(r):
            for p in range(PAIR):
                body(base + r * PAIR + p)

        loop(HG // PAIR, one)

    def units(first, n, body):
        def one(r):
            for p in range(PAIR):
                body((first + r) * PAIR + p)

        loop(n, one)

    def others(body):
        lax.fori_loop(1, NC, lambda r, c: (body(lax.rem(chip + r, NC)), c)[1], 0)

    loads = [
        pltpu.make_async_copy(src, dst, in_sem.at[n])
        for n, (src, dst) in enumerate(((k_in, k), (v_in, v), (q_in, q), (g_in, g)))
    ]
    loads[0].start()
    loads[1].start()

    barrier = pltpu.get_barrier_semaphore()
    others(
        lambda i: pl.semaphore_signal(barrier, inc=1, device_id=at(i), device_id_type=MESH)
    )
    pl.semaphore_signal(barrier, inc=1, device_id=mate, device_id_type=MESH)
    for r in range(1, NY):
        pl.semaphore_signal(
            barrier, inc=1, device_id={"head": lax.rem(y + r, NY)}, device_id_type=MESH
        )

    row_i = lax.broadcasted_iota(jnp.int32, (DH, DH), 0)
    col_i = lax.broadcasted_iota(jnp.int32, (DH, DH), 1)
    lower = row_i >= col_i
    tri = jnp.where(lower, 1.0, 0.0).astype(F32)

    total = jnp.zeros((H, 1), F32)
    for j in range(NJ):
        piece = ld[:, j * DH:(j + 1) * DH]
        rows = exact_nt(piece, tri)
        columns = exact_nt(tri, piece)
        for h in range(H):
            rc[h, :, j * DH:(j + 1) * DH] = rows[h:h + 1, :]
            cb[h, j * DH:(j + 1) * DH, :] = jnp.broadcast_to(columns[:, h:h + 1], (DH, DH))
        total = total + rows[:, DH - 1:DH]
    dec_own[...] = jnp.broadcast_to(total, (H, DH)).reshape(H, 1, DH)
    loads[2].start()
    loads[3].start()

    def cums(h, j):
        return cb[h, j * DH:(j + 1) * DH, :]

    def cum_row(h, j):
        return rc[h, :, j * DH:(j + 1) * DH]

    def local_states(h):
        state = None
        for j in range(NJ):
            row = cum_row(h, j)
            end = row[:, DH - 1:DH]
            flipped = tile(k, h, j).T
            put(kt, h, j, flipped)
            scaled = (flipped.astype(F32) * jnp.exp(end - row)).astype(BF16)
            part = nn(scaled, tile(v, h, j))
            ms[h, j] = part
            last = jnp.exp(cb[h, j * DH + DH - 1:j * DH + DH, :])
            state = part if state is None else last * state + part
        loc[h] = state

    def group(ref, base, n):
        return ref.at[pl.ds(base + n * HG, HG)]

    def swap(src, recv, s, r, n):
        return remote(group(src, oth0, n), recv.at[n], s.at[n], r.at[n], mate)

    def give(dst, s, r, n, base):
        return remote(pst.at[n], group(dst, base, n), s.at[n], r.at[n], mate)

    def scan_total(first, recv, n):
        def one(r):
            h = own0 + n * HG + r
            mine = jnp.where(first, jnp.exp(dec_par[h]), 1.0)
            theirs = jnp.where(first, 1.0, jnp.exp(dec_own[h]))
            tot[n, pl.ds(pl.multiple_of(r * DH, DH), DH), :] = mine * loc[h] + theirs * recv[n, r]

        loop(HG, one)

    side = 4 if NC == 16 else 2
    steps = [(a, b) for a in range(side) for b in range(side) if a + b > 0]
    steps.sort(key=lambda ab: -sum(min(d, side - d) for d in ab))

    def farthest(body):
        for a, b in steps:
            body(lax.rem(chip // side + a, side) * side + lax.rem(chip % side + b, side))

    def piece_of(ref, n, i):
        return ref.at[n, pl.ds(pl.multiple_of(i * RS, RS), RS), :]

    def send_out(recv, s, r, n):
        farthest(
            lambda i: remote(piece_of(tot, n, i), recv.at[n, chip], s.at[n], r.at[n], at(i)).start()
        )

    def all_out(recv, s, r, n):
        return remote(
            tot.at[n, pl.ds(0, (NC - 1) * RS), :], tot.at[n, pl.ds(0, (NC - 1) * RS), :],
            s.at[n], r.at[n], mate,
        )

    def all_in(recv, s, r, n):
        part = recv.at[n, pl.ds(0, NC - 1)]
        return remote(part, part, s.at[n], r.at[n], mate)

    def send_back(dst, s, r, n):
        farthest(
            lambda i: remote(px.at[n, i], piece_of(dst, n, chip), s.at[n], r.at[n], at(i)).start()
        )

    def all_back(s, r, n):
        part = px.at[n, pl.ds(0, NC - 1)]
        return remote(part, part, s.at[n], r.at[n], mate)

    def all_home(dst, s, r, n):
        part = dst.at[n, pl.ds(0, (NC - 1) * RS), :]
        return remote(part, part, s.at[n], r.at[n], mate)

    def prefix(recv, dst, s, r, n, reverse):
        head = own0 + n * HG + (chip * RS) // DH
        mine = pl.ds(pl.multiple_of(chip * RS, RS), RS)
        recv[n, chip] = tot[n, mine, :]
        all_in(recv, s, r, n).wait_recv()
        state = jnp.zeros((RS, DH), F32)
        for i in reversed(range(NC)) if reverse else range(NC):
            px[n, i] = state
            state = jnp.exp(dec_all[i, head]) * state + recv[n, i]
        dst[n, mine, :] = px[n, chip]

    def settle(first, homed, recv, dst, n):
        def one(r):
            h = own0 + n * HG + r
            state = homed[n, pl.ds(pl.multiple_of(r * DH, DH), DH), :]
            ahead = jnp.where(first, 1.0, jnp.exp(dec_par[h]))
            dst[h] = ahead * state + jnp.where(first, 0.0, recv[n, r])
            after = jnp.where(first, jnp.exp(dec_own[h]), 1.0)
            pst[n, r] = after * state + jnp.where(first, loc[h], 0.0)

        loop(HG, one)

    dec_copy = remote(dec_own, dec_par, dp_s.at[0], dp_r.at[0], mate)

    def dec_send(i):
        return remote(dec_chip, dec_all.at[chip], da_s.at[0], da_r.at[0], at(i))

    dec_part = dec_all.at[pl.ds(0, NC - 1)]
    dec_done = remote(dec_part, dec_part, da_s.at[0], da_r.at[0], mate)

    loads[0].wait()
    loads[1].wait()
    heads(oth0, local_states)
    pl.semaphore_wait(barrier, NC - 1 + 1 + NY - 1)
    dec_copy.start()
    swap(loc, lpr, lp_s, lp_r, 0).start()

    def for_mate(n):
        heads(oth0 + n * HG, local_states)
        swap(loc, lpr, lp_s, lp_r, n).start()

    span(1, G, for_mate)
    dec_copy.wait()
    dec_chip[...] = dec_own[...] + dec_par[...]
    dec_all[chip] = dec_chip[...]
    others(lambda i: dec_send(i).start())

    def for_own(n):
        heads(own0 + n * HG, local_states)
        swap(loc, lpr, lp_s, lp_r, n).wait()
        scan_total(core == 0, lpr, n)
        send_out(rx, rx_s, rx_r, n)

    loop(G, for_own)

    loads[2].wait()

    def intra(h):
        for j in range(NJ):
            qj, vj = tile(q, h, j), tile(v, h, j)
            decay = jnp.exp(jnp.where(lower, cums(h, j) - cum_row(h, j), -jnp.inf))
            weights = (nn(qj, tile(kt, h, j)) * decay).astype(BF16)
            put(att, h, j, nn(weights, vj))
            put(wt, h, j, weights.T)
            lifted = qj.T.astype(F32) * jnp.exp(cum_row(h, j))
            put(ga, h, j, lifted.astype(BF16))
            put(kt, h, j, vj.T)

    ahead = U // 4
    units(0, ahead, intra)
    dec_done.wait()

    def forward(n):
        prefix(rx, pin, rx_s, rx_r, n, False)
        send_back(pin, pi_s, pi_r, n)
        units(ahead + n, 1, intra)

    loop(G, forward)
    units(ahead + G, U - ahead - G, intra)
    loads[3].wait()
    acc_s[...] = jnp.zeros_like(acc_s)
    acc_c[...] = jnp.zeros_like(acc_c)

    def inter(h):
        states = [st[h + p] for p in range(PAIR)]
        scales = [gain[:, pl.ds(pl.multiple_of((h + p) * DH, DH), DH)] for p in range(PAIR)]
        for j in range(NJ):
            squares, crosses = None, None
            for p in range(PAIR):
                cum = cums(h + p, j)
                low = states[p].astype(BF16)
                sbf[h + p, j] = low
                mixed = tile(att, h + p, j) + jnp.exp(cum) * nn(tile(q, h + p, j), low)
                put(att, h + p, j, mixed)
                square = mixed * mixed
                cross = tile(g, h + p, j).astype(F32) * scales[p] * mixed
                squares = square if squares is None else squares + square
                crosses = cross if crosses is None else crosses + cross
                if j < NJ - 1:
                    states[p] = jnp.exp(cum[DH - 1:DH, :]) * states[p] + ms[h + p, j]
            acc_s[j * DH:(j + 1) * DH, :] += squares
            acc_c[j * DH:(j + 1) * DH, :] += crosses

    def mine(n):
        all_home(pin, pi_s, pi_r, n).wait_recv()
        settle(core == 0, pin, lpr, st, n)
        give(st, ps_s, ps_r, n, own0).start()
        loop(HG // PAIR, lambda r: inter(own0 + n * HG + r * PAIR))

    def theirs(n):
        give(st, ps_s, ps_r, n, oth0).wait_recv()
        loop(HG // PAIR, lambda r: inter(oth0 + n * HG + r * PAIR))

    loop(G, mine)
    loop(G, theirs)

    pick = lax.broadcasted_iota(jnp.int32, (8, DH), 0) == 0
    for j in range(NJ):
        a = jnp.sum(acc_s[j * DH:(j + 1) * DH, :].T, axis=0, keepdims=True)
        b = jnp.sum(acc_c[j * DH:(j + 1) * DH, :].T, axis=0, keepdims=True)
        sums[:, j * DH:(j + 1) * DH] = jnp.where(pick, a, b)
    for r in range(1, NY):
        d = lax.rem(y + r, NY)
        remote(sums, hx.at[y], hx_s.at[0], hx_r.at[0], {"head": d}).start()
    hx[y] = sums[...]

    def turn(h):
        for j in range(NJ):
            sbf[h, j] = sbf[h, j].T

    units(0, U, turn)

    def sent(n):
        all_out(rx, rx_s, rx_r, n).wait_send()
        all_back(pi_s, pi_r, n).wait_send()
        give(st, ps_s, ps_r, n, own0).wait_send()

    loop(G, sent)
    hx_part = hx.at[pl.ds(0, NY - 1)]
    remote(hx_part, hx_part, hx_s.at[0], hx_r.at[0], mate).wait()
    for j in range(NJ):
        both = hx[0, :, j * DH:(j + 1) * DH]
        for r in range(1, NY):
            both = both + hx[r, :, j * DH:(j + 1) * DH]
        inverse = lax.rsqrt(both[0:1, :] / HD + EPSILON)
        center = both[1:2, :] * inverse / HD
        columns = jnp.where(pick, inverse, center).T
        acc_s[j * DH:(j + 1) * DH, :] = jnp.broadcast_to(columns[:, 0:1], (DH, DH))
        acc_c[j * DH:(j + 1) * DH, :] = jnp.broadcast_to(columns[:, 1:2], (DH, DH))

    def normalize(h):
        scale = gain[:, pl.ds(pl.multiple_of(h * DH, DH), DH)]
        gain_part = jnp.zeros((8, DH), F32)
        for j in range(NJ):
            inverse = acc_s[j * DH:(j + 1) * DH, :]
            normed = tile(att, h, j) * inverse
            grad = tile(g, h, j).astype(F32)
            put(g, h, j, (normed * scale).astype(BF16))
            gain_part = gain_part + jnp.sum((grad * normed).reshape(DH // 8, 8, DH), axis=0)
            center = acc_c[j * DH:(j + 1) * DH, :]
            low = (inverse * (grad * scale - normed * center)).astype(BF16)
            ms[h, j] = nn(tile(ga, h, j), low)
            put(ga, h, j, low)
        ggp[h] = gain_part
        state = ms[h, NJ - 1]
        for j in range(NJ - 2, -1, -1):
            end = cb[h, j * DH + DH - 1:j * DH + DH, :]
            state = jnp.exp(end) * state + ms[h, j]
        loc[h] = state

    def grads_mate(n):
        heads(oth0 + n * HG, normalize)
        swap(loc, lpr, glp_s, glp_r, n).start()

    def grads_own(n):
        heads(own0 + n * HG, normalize)
        swap(loc, lpr, glp_s, glp_r, n).wait()
        scan_total(core == 1, lpr, n)
        send_out(rx, grx_s, grx_r, n)

    loop(G, grads_mate)
    loop(G, grads_own)

    gain_copy = remote(ggp, ggpr, gp_s.at[0], gp_r.at[0], mate)
    gain_copy.start()

    def intra_grads(h):
        for j in range(NJ):
            gj = tile(ga, h, j)
            cum = cums(h, j)
            decay = jnp.exp(jnp.where(lower, cum - cum_row(h, j), -jnp.inf))
            gw = (nn(gj, tile(kt, h, j)) * decay).astype(BF16)
            grown = (gj.astype(F32) * jnp.exp(cum)).astype(BF16)
            gq = nn(gw, tile(k, h, j)) + nn(grown, sbf[h, j])
            put(gvi, h, j, nn(tile(wt, h, j), gj))
            put(att, h, j, nn(gw.T, tile(q, h, j)))
            put(q, h, j, gq.astype(BF16))

    soon = U // 4
    units(0, soon, intra_grads)
    gain_copy.wait()
    ggc[...] = ggp[...] + ggpr[...]
    ggrx[chip] = ggc[chip]
    others(lambda i: remote(ggc.at[i], ggrx.at[chip], gr_s.at[0], gr_r.at[0], at(i)).start())

    def backward(n):
        prefix(rx, pin, grx_s, grx_r, n, True)
        send_back(pin, gpi_s, gpi_r, n)

    backward(0)
    units(soon, 1, intra_grads)
    span(1, G, backward)
    units(soon + 1, U - soon - 2, intra_grads)
    gr_part = ggrx.at[pl.ds(0, NC - 1)]
    remote(gr_part, gr_part, gr_s.at[0], gr_r.at[0], mate).wait()
    part = ggrx[0]
    for i in range(1, NC):
        part = part + ggrx[i]
    ggsum[...] = part
    ggall[chip] = part
    others(lambda i: remote(ggsum, ggall.at[chip], ga_s.at[0], ga_r.at[0], at(i)).start())

    def later_states(h):
        state = st[h]
        for j in range(NJ - 1, -1, -1):
            sbf[h, j] = state.astype(BF16)
            if j > 0:
                state = jnp.exp(cb[h, j * DH + DH - 1:j * DH + DH, :]) * state + ms[h, j]

    def last_mine(n):
        all_home(pin, gpi_s, gpi_r, n).wait_recv()
        settle(core == 1, pin, lpr, st, n)
        give(st, gps_s, gps_r, n, own0).start()

    def last_theirs(n):
        give(st, gps_s, gps_r, n, oth0).wait_recv()
        heads(oth0 + n * HG, later_states)

    loop(G, last_mine)
    units(U - 1, 1, intra_grads)
    loop(G, lambda n: heads(own0 + n * HG, later_states))
    loop(G, last_theirs)

    gg_part = ggall.at[pl.ds(0, NC - 1)]
    remote(gg_part, gg_part, ga_s.at[0], ga_r.at[0], mate).wait()
    for h in range(H):
        gg_out[h:h + 1, :] = jnp.sum(ggall[h], axis=0, keepdims=True)
    def done(n):
        all_out(rx, grx_s, grx_r, n).wait_send()
        all_back(gpi_s, gpi_r, n).wait_send()
        give(st, gps_s, gps_r, n, own0).wait_send()

    loop(G, done)


def on_device(sizes, queries, key_rows, value_rows, log_decay, norm_gain, grad_out):
    T, H, NC, NY = sizes
    W = H * DH
    NJ = T // DH
    HH = H // 2
    G = groups_of(HH)
    HG = HH // G
    RS = HG * DH // NC
    V = pltpu.VMEM
    D = pltpu.SemaphoreType.DMA
    rows = V((G, HG * DH, DH), F32)
    slots = V((G, NC, RS, DH), F32)
    heads = V((G, HG, DH, DH), F32)
    states = V((H, DH, DH), F32)
    scratch = [
        V((H, 1, T), F32), V((H, NJ, DH, DH), F32), V((T, W), BF16), V((T, W), BF16),
        V((T, W), BF16),
        V((T, DH), F32), V((T, DH), F32),
        V((8, T), F32), V((NY, 8, T), F32),
        V((H, 1, DH), F32), V((H, 1, DH), F32), V((H, 1, DH), F32), V((NC, H, 1, DH), F32),
        states, rows, slots, heads, heads, slots, rows, states,
        V((H, 8, DH), F32), V((H, 8, DH), F32), V((H, 8, DH), F32), V((NC, 8, DH), F32),
        V((8, DH), F32), V((NC, 8, DH), F32),
        D((4,)), *[D((1,))] * 6, *[D((G,))] * 16, *[D((1,))] * 6,
    ]
    anywhere = pl.BlockSpec(memory_space=pl.ANY)
    local = pl.BlockSpec(memory_space=V)
    held = (
        V((T, W), BF16), V((T, W), BF16), V((T, W), BF16), V((T, W), BF16),
        V((H, T, DH), F32), V((H, NJ, DH, DH), BF16), V((T, W), F32), V((T, W), F32),
        V((H, DH), F32),
    )
    parts = pl.pallas_call(
        functools.partial(kernel, sizes),
        out_shape=held,
        in_specs=[anywhere, anywhere, anywhere, local, local, anywhere],
        out_specs=(local,) * len(held),
        scratch_shapes=scratch,
        compiler_params=pltpu.CompilerParams(
            collective_id=0, has_side_effects=True, vmem_limit_bytes=23 << 20
        ),
    )(queries, key_rows, value_rows, log_decay, norm_gain.reshape(1, W), grad_out)
    parts = [pltpu.with_memory_space_constraint(x, V) for x in parts]
    big = jax.ShapeDtypeStruct((T, W), BF16)
    *grads, gain_grad = pl.pallas_call(
        functools.partial(finish, sizes),
        out_shape=(big, big, big, big, jax.ShapeDtypeStruct((H, DH), F32)),
        in_specs=[local] * len(held),
        out_specs=(anywhere, anywhere, anywhere, anywhere, local),
        scratch_shapes=[
            V((T, W), BF16), V((T, W), BF16), D((2,)), D((2, H)),
        ],
        compiler_params=pltpu.CompilerParams(vmem_limit_bytes=9 << 20),
    )(*parts)
    return (*grads, gain_grad.reshape(W))


def solution(mesh):
    def whole(queries, key_rows, value_rows, log_decay, norm_gain, grad_out):
        seq, head = mesh.shape["seq"], mesh.shape["head"]
        sizes = (queries.shape[0] // seq, queries.shape[1] // DH // head, seq // 2, head)
        rows = P("seq", "head")
        return jax.shard_map(
            functools.partial(on_device, sizes),
            mesh=mesh,
            in_specs=(rows, rows, rows, P("head", "seq"), P("head"), rows),
            out_specs=(rows, rows, rows, rows, P("head")),
            check_vma=False,
        )(queries, key_rows, value_rows, log_decay, norm_gain, grad_out)

    return whole
```

```python
import functools

import jax
import jax.numpy as jnp
from jax import lax
from jax.experimental import pallas as pl
from jax.experimental.pallas import tpu as pltpu
from jax.sharding import PartitionSpec as P

DH = 128
EPSILON = 1e-06
F32 = jnp.float32
BF16 = jnp.bfloat16
MESH = pl.DeviceIdType.MESH
HIGHEST = lax.Precision.HIGHEST


def groups_of(heads):
    return 4 if heads % 8 == 0 else 2


def nn(a, b):
    return lax.dot_general(a, b, (((1,), (0,)), ((), ())), preferred_element_type=F32)


def nt(a, b):
    return lax.dot_general(a, b, (((1,), (1,)), ((), ())), preferred_element_type=F32)


def tn(a, b):
    return lax.dot_general(a, b, (((0,), (0,)), ((), ())), preferred_element_type=F32)


def exact_nt(a, b):
    return lax.dot_general(
        a, b, (((1,), (1,)), ((), ())), preferred_element_type=F32, precision=HIGHEST
    )


def tile(ref, h, j):
    return ref[j * DH:(j + 1) * DH, pl.ds(pl.multiple_of(h * DH, DH), DH)]


def put(ref, h, j, value):
    ref[j * DH:(j + 1) * DH, pl.ds(pl.multiple_of(h * DH, DH), DH)] = value


def inter_grads(sizes, h, k, v, cb, sbf, att, gvi, gk, gv):
    for j in range(sizes[0] // DH):
        cum = cb[h, j * DH:(j + 1) * DH, :]
        low = sbf[h, j]
        tail = jnp.exp(cum[DH - 1:DH, :] - cum)
        kj, vj = tile(k, h, j), tile(v, h, j)
        put(gk, h, j, (tile(att, h, j) + tail * nn(vj, low.T)).astype(BF16))
        put(gv, h, j, (tile(gvi, h, j) + tail * nn(kj, low)).astype(BF16))


def finish(
    sizes,
    q, k, v, g, cb, sbf, att, gvi, gg,
    out_hbm, gq_hbm, gk_hbm, gv_hbm, gg_out,
    gk, gv, sem, head_sem,
):
    H = sizes[1]
    copies = [
        pltpu.make_async_copy(src, dst, sem.at[n])
        for n, (src, dst) in enumerate(((g, out_hbm), (q, gq_hbm)))
    ]
    for c in copies:
        c.start()
    gg_out[...] = gg[...]

    def stores(h):
        columns = pl.ds(pl.multiple_of(h * DH, DH), DH)
        return [
            pltpu.make_async_copy(a.at[:, columns], b.at[:, columns], head_sem.at[n, h])
            for n, (a, b) in enumerate(((gk, gk_hbm), (gv, gv_hbm)))
        ]

    def one(h, carry):
        inter_grads(sizes, h, k, v, cb, sbf, att, gvi, gk, gv)
        for c in stores(h):
            c.start()
        return carry

    def ended(h, carry):
        for c in stores(h):
            c.wait()
        return carry

    lax.fori_loop(0, H, one, 0)
    lax.fori_loop(0, H, ended, 0)
    for c in copies:
        c.wait()


def kernel(
    sizes,
    q_in, k_in, v_in, ld, gain, g_in,
    q, k, v, g, cb, sbf, att, gvi, gg_out,
    rc, ms, ga, kt, wt,
    acc_s, acc_c, sums, hx,
    dec_own, dec_par, dec_chip, dec_all,
    loc, tot, px, pst, lpr, rx, pin, st,
    ggp, ggpr, ggc, ggrx, ggsum, ggall,
    in_sem, dp_s, dp_r, da_s, da_r, hx_s, hx_r,
    lp_s, lp_r, rx_s, rx_r, pi_s, pi_r, ps_s, ps_r,
    glp_s, glp_r, grx_s, grx_r, gpi_s, gpi_r, gps_s, gps_r,
    gp_s, gp_r, gr_s, gr_r, ga_s, ga_r,
):
    T, H, NC, NY = sizes
    NJ = T // DH
    HH = H // 2
    G = groups_of(HH)
    HG = HH // G
    RS = HG * DH // NC
    HD = NY * H * DH
    PAIR = 2 if HG % 2 == 0 else 1
    U = H // PAIR
    me = lax.axis_index("seq")
    y = lax.axis_index("head")
    chip = me // 2
    core = me % 2
    mate = {"seq": chip * 2 + (1 - core)}
    own0 = core * HH
    oth0 = (1 - core) * HH

    def at(i):
        return {"seq": i * 2 + core}

    def remote(src, dst, s, r, dev):
        return pltpu.make_async_remote_copy(
            src_ref=src, dst_ref=dst, send_sem=s, recv_sem=r, device_id=dev, device_id_type=MESH
        )

    def loop(n, body):
        lax.fori_loop(0, n, lambda i, c: (body(i), c)[1], 0)

    def span(first, n, body):
        lax.fori_loop(first, n, lambda i, c: (body(i), c)[1], 0)

    def heads(base, body):
        def one(r):
            for p in range(PAIR):
                body(base + r * PAIR + p)

        loop(HG // PAIR, one)

    def units(first, n, body):
        def one(r):
            for p in range(PAIR):
                body((first + r) * PAIR + p)

        loop(n, one)

    def others(body):
        lax.fori_loop(1, NC, lambda r, c: (body(lax.rem(chip + r, NC)), c)[1], 0)

    near = pl.ds(pl.multiple_of(oth0 * DH, HH * DH), HH * DH)
    late = pl.ds(pl.multiple_of(own0 * DH, HH * DH), HH * DH)
    loads = [
        pltpu.make_async_copy(src, dst, in_sem.at[n])
        for n, (src, dst) in enumerate((
            (k_in.at[:, near], k.at[:, near]), (v_in.at[:, near], v.at[:, near]),
            (k_in.at[:, late], k.at[:, late]), (v_in.at[:, late], v.at[:, late]),
            (q_in, q), (g_in, g),
        ))
    ]
    for c in loads[:4]:
        c.start()

    barrier = pltpu.get_barrier_semaphore()
    others(
        lambda i: pl.semaphore_signal(barrier, inc=1, device_id=at(i), device_id_type=MESH)
    )
    pl.semaphore_signal(barrier, inc=1, device_id=mate, device_id_type=MESH)
    for r in range(1, NY):
        pl.semaphore_signal(
            barrier, inc=1, device_id={"head": lax.rem(y + r, NY)}, device_id_type=MESH
        )

    row_i = lax.broadcasted_iota(jnp.int32, (DH, DH), 0)
    col_i = lax.broadcasted_iota(jnp.int32, (DH, DH), 1)
    lower = row_i >= col_i
    tri = jnp.where(lower, 1.0, 0.0).astype(F32)

    total = jnp.zeros((H, 1), F32)
    for j in range(NJ):
        piece = ld[:, j * DH:(j + 1) * DH]
        rows = exact_nt(piece, tri)
        acc_c[j * DH:(j + 1) * DH, 0:H] = exact_nt(tri, piece)
        for h in range(H):
            rc[h, :, j * DH:(j + 1) * DH] = rows[h:h + 1, :]
        total = total + rows[:, DH - 1:DH]
    dec_own[...] = jnp.broadcast_to(total, (H, DH)).reshape(H, 1, DH)
    for c in loads[4:]:
        c.start()

    def cums(h, j):
        return cb[h, j * DH:(j + 1) * DH, :]

    def cum_row(h, j):
        return rc[h, :, j * DH:(j + 1) * DH]

    def local_states(h):
        state = None
        for j in range(NJ):
            row = cum_row(h, j)
            end = row[:, DH - 1:DH]
            flipped = tile(k, h, j).T
            put(kt, h, j, flipped)
            scaled = (flipped.astype(F32) * jnp.exp(end - row)).astype(BF16)
            part = nn(scaled, tile(v, h, j))
            ms[h, j] = part
            last = jnp.broadcast_to(jnp.exp(end), (1, DH))
            state = part if state is None else last * state + part
        loc[h] = state

    def group(ref, base, n):
        return ref.at[pl.ds(base + n * HG, HG)]

    def swap(src, recv, s, r, n):
        return remote(group(src, oth0, n), recv.at[n], s.at[n], r.at[n], mate)

    def give(dst, s, r, n, base):
        return remote(pst.at[n], group(dst, base, n), s.at[n], r.at[n], mate)

    def scan_total(first, recv, n):
        def one(r):
            h = own0 + n * HG + r
            mine = jnp.where(first, jnp.exp(dec_par[h]), 1.0)
            theirs = jnp.where(first, 1.0, jnp.exp(dec_own[h]))
            tot[n, pl.ds(pl.multiple_of(r * DH, DH), DH), :] = mine * loc[h] + theirs * recv[n, r]

        loop(HG, one)

    side = 4 if NC == 16 else 2
    steps = [(a, b) for a in range(side) for b in range(side) if a + b > 0]
    steps.sort(key=lambda ab: -sum(min(d, side - d) for d in ab))

    def farthest(body):
        for a, b in steps:
            body(lax.rem(chip // side + a, side) * side + lax.rem(chip % side + b, side))

    def piece_of(ref, n, i):
        return ref.at[n, pl.ds(pl.multiple_of(i * RS, RS), RS), :]

    def send_out(recv, s, r, n):
        farthest(
            lambda i: remote(piece_of(tot, n, i), recv.at[n, chip], s.at[n], r.at[n], at(i)).start()
        )

    def all_out(recv, s, r, n):
        return remote(
            tot.at[n, pl.ds(0, (NC - 1) * RS), :], tot.at[n, pl.ds(0, (NC - 1) * RS), :],
            s.at[n], r.at[n], mate,
        )

    def all_in(recv, s, r, n):
        part = recv.at[n, pl.ds(0, NC - 1)]
        return remote(part, part, s.at[n], r.at[n], mate)

    def send_back(dst, s, r, n):
        farthest(
            lambda i: remote(px.at[n, i], piece_of(dst, n, chip), s.at[n], r.at[n], at(i)).start()
        )

    def all_back(s, r, n):
        part = px.at[n, pl.ds(0, NC - 1)]
        return remote(part, part, s.at[n], r.at[n], mate)

    def all_home(dst, s, r, n):
        part = dst.at[n, pl.ds(0, (NC - 1) * RS), :]
        return remote(part, part, s.at[n], r.at[n], mate)

    def prefix(recv, dst, s, r, n, reverse):
        head = own0 + n * HG + (chip * RS) // DH
        mine = pl.ds(pl.multiple_of(chip * RS, RS), RS)
        recv[n, chip] = tot[n, mine, :]
        all_in(recv, s, r, n).wait_recv()
        state = jnp.zeros((RS, DH), F32)
        for i in reversed(range(NC)) if reverse else range(NC):
            px[n, i] = state
            state = jnp.exp(dec_all[i, head]) * state + recv[n, i]
        dst[n, mine, :] = px[n, chip]

    def settle(first, homed, recv, dst, n):
        def one(r):
            h = own0 + n * HG + r
            state = homed[n, pl.ds(pl.multiple_of(r * DH, DH), DH), :]
            ahead = jnp.where(first, 1.0, jnp.exp(dec_par[h]))
            dst[h] = ahead * state + jnp.where(first, 0.0, recv[n, r])
            after = jnp.where(first, jnp.exp(dec_own[h]), 1.0)
            pst[n, r] = after * state + jnp.where(first, loc[h], 0.0)

        loop(HG, one)

    dec_copy = remote(dec_own, dec_par, dp_s.at[0], dp_r.at[0], mate)

    def dec_send(i):
        return remote(dec_chip, dec_all.at[chip], da_s.at[0], da_r.at[0], at(i))

    dec_part = dec_all.at[pl.ds(0, NC - 1)]
    dec_done = remote(dec_part, dec_part, da_s.at[0], da_r.at[0], mate)

    loads[0].wait()
    loads[1].wait()
    heads(oth0, local_states)
    pl.semaphore_wait(barrier, NC - 1 + 1 + NY - 1)
    dec_copy.start()
    swap(loc, lpr, lp_s, lp_r, 0).start()

    def for_mate(n):
        heads(oth0 + n * HG, local_states)
        swap(loc, lpr, lp_s, lp_r, n).start()

    span(1, G, for_mate)
    dec_copy.wait()
    dec_chip[...] = dec_own[...] + dec_par[...]
    dec_all[chip] = dec_chip[...]
    others(lambda i: dec_send(i).start())

    def for_own(n):
        heads(own0 + n * HG, local_states)
        swap(loc, lpr, lp_s, lp_r, n).wait()
        scan_total(core == 0, lpr, n)
        send_out(rx, rx_s, rx_r, n)

    loads[2].wait()
    loads[3].wait()
    loop(G, for_own)
    for j in range(NJ):
        columns = acc_c[j * DH:(j + 1) * DH, 0:H]
        for h in range(H):
            cb[h, j * DH:(j + 1) * DH, :] = jnp.broadcast_to(columns[:, h:h + 1], (DH, DH))

    loads[4].wait()

    def intra(h):
        for j in range(NJ):
            qj, vj = tile(q, h, j), tile(v, h, j)
            decay = jnp.exp(jnp.where(lower, cums(h, j) - cum_row(h, j), -jnp.inf))
            weights = (nn(qj, tile(kt, h, j)) * decay).astype(BF16)
            put(att, h, j, nn(weights, vj))
            put(wt, h, j, weights.T)
            lifted = qj.T.astype(F32) * jnp.exp(cum_row(h, j))
            put(ga, h, j, lifted.astype(BF16))
            put(kt, h, j, vj.T)

    ahead = U // 4
    units(0, ahead, intra)
    dec_done.wait()

    def forward(n):
        prefix(rx, pin, rx_s, rx_r, n, False)
        send_back(pin, pi_s, pi_r, n)
        units(ahead + n, 1, intra)

    loop(G, forward)
    units(ahead + G, U - ahead - G, intra)
    loads[5].wait()
    acc_s[...] = jnp.zeros_like(acc_s)
    acc_c[...] = jnp.zeros_like(acc_c)

    def inter(h):
        states = [st[h + p] for p in range(PAIR)]
        scales = [gain[:, pl.ds(pl.multiple_of((h + p) * DH, DH), DH)] for p in range(PAIR)]
        for j in range(NJ):
            squares, crosses = None, None
            for p in range(PAIR):
                cum = cums(h + p, j)
                low = states[p].astype(BF16)
                sbf[h + p, j] = low
                mixed = tile(att, h + p, j) + jnp.exp(cum) * nn(tile(q, h + p, j), low)
                put(att, h + p, j, mixed)
                square = mixed * mixed
                cross = tile(g, h + p, j).astype(F32) * scales[p] * mixed
                squares = square if squares is None else squares + square
                crosses = cross if crosses is None else crosses + cross
                if j < NJ - 1:
                    states[p] = jnp.exp(cum[DH - 1:DH, :]) * states[p] + ms[h + p, j]
            acc_s[j * DH:(j + 1) * DH, :] += squares
            acc_c[j * DH:(j + 1) * DH, :] += crosses

    def mine(n):
        all_home(pin, pi_s, pi_r, n).wait_recv()
        settle(core == 0, pin, lpr, st, n)
        give(st, ps_s, ps_r, n, own0).start()
        loop(HG // PAIR, lambda r: inter(own0 + n * HG + r * PAIR))

    def theirs(n):
        give(st, ps_s, ps_r, n, oth0).wait_recv()
        loop(HG // PAIR, lambda r: inter(oth0 + n * HG + r * PAIR))

    loop(G, mine)
    loop(G, theirs)

    pick = lax.broadcasted_iota(jnp.int32, (8, DH), 0) == 0
    for j in range(NJ):
        a = jnp.sum(acc_s[j * DH:(j + 1) * DH, :].T, axis=0, keepdims=True)
        b = jnp.sum(acc_c[j * DH:(j + 1) * DH, :].T, axis=0, keepdims=True)
        sums[:, j * DH:(j + 1) * DH] = jnp.where(pick, a, b)
    for r in range(1, NY):
        d = lax.rem(y + r, NY)
        remote(sums, hx.at[y], hx_s.at[0], hx_r.at[0], {"head": d}).start()
    hx[y] = sums[...]

    def turn(h):
        for j in range(NJ):
            sbf[h, j] = sbf[h, j].T

    units(0, U, turn)

    def sent(n):
        all_out(rx, rx_s, rx_r, n).wait_send()
        all_back(pi_s, pi_r, n).wait_send()
        give(st, ps_s, ps_r, n, own0).wait_send()

    loop(G, sent)
    hx_part = hx.at[pl.ds(0, NY - 1)]
    remote(hx_part, hx_part, hx_s.at[0], hx_r.at[0], mate).wait()
    for j in range(NJ):
        both = hx[0, :, j * DH:(j + 1) * DH]
        for r in range(1, NY):
            both = both + hx[r, :, j * DH:(j + 1) * DH]
        inverse = lax.rsqrt(both[0:1, :] / HD + EPSILON)
        center = both[1:2, :] * inverse / HD
        columns = jnp.where(pick, inverse, center).T
        acc_s[j * DH:(j + 1) * DH, :] = jnp.broadcast_to(columns[:, 0:1], (DH, DH))
        acc_c[j * DH:(j + 1) * DH, :] = jnp.broadcast_to(columns[:, 1:2], (DH, DH))

    def normalize(h):
        scale = gain[:, pl.ds(pl.multiple_of(h * DH, DH), DH)]
        gain_part = jnp.zeros((8, DH), F32)
        for j in range(NJ):
            inverse = acc_s[j * DH:(j + 1) * DH, :]
            normed = tile(att, h, j) * inverse
            grad = tile(g, h, j).astype(F32)
            put(g, h, j, (normed * scale).astype(BF16))
            gain_part = gain_part + jnp.sum((grad * normed).reshape(DH // 8, 8, DH), axis=0)
            center = acc_c[j * DH:(j + 1) * DH, :]
            low = (inverse * (grad * scale - normed * center)).astype(BF16)
            ms[h, j] = nn(tile(ga, h, j), low)
            put(ga, h, j, low)
        ggp[h] = gain_part
        state = ms[h, NJ - 1]
        for j in range(NJ - 2, -1, -1):
            end = cb[h, j * DH + DH - 1:j * DH + DH, :]
            state = jnp.exp(end) * state + ms[h, j]
        loc[h] = state

    def grads_mate(n):
        heads(oth0 + n * HG, normalize)
        swap(loc, lpr, glp_s, glp_r, n).start()

    def grads_own(n):
        heads(own0 + n * HG, normalize)
        swap(loc, lpr, glp_s, glp_r, n).wait()
        scan_total(core == 1, lpr, n)
        send_out(rx, grx_s, grx_r, n)

    loop(G, grads_mate)
    loop(G, grads_own)

    gain_copy = remote(ggp, ggpr, gp_s.at[0], gp_r.at[0], mate)
    gain_copy.start()

    def intra_grads(h):
        for j in range(NJ):
            gj = tile(ga, h, j)
            cum = cums(h, j)
            decay = jnp.exp(jnp.where(lower, cum - cum_row(h, j), -jnp.inf))
            gw = (nn(gj, tile(kt, h, j)) * decay).astype(BF16)
            grown = (gj.astype(F32) * jnp.exp(cum)).astype(BF16)
            gq = nn(gw, tile(k, h, j)) + nn(grown, sbf[h, j])
            put(gvi, h, j, nn(tile(wt, h, j), gj))
            put(att, h, j, nn(gw.T, tile(q, h, j)))
            put(q, h, j, gq.astype(BF16))

    soon = U // 4
    units(0, soon, intra_grads)
    gain_copy.wait()
    ggc[...] = ggp[...] + ggpr[...]
    ggrx[chip] = ggc[chip]
    others(lambda i: remote(ggc.at[i], ggrx.at[chip], gr_s.at[0], gr_r.at[0], at(i)).start())

    def backward(n):
        prefix(rx, pin, grx_s, grx_r, n, True)
        send_back(pin, gpi_s, gpi_r, n)

    backward(0)
    units(soon, 1, intra_grads)
    span(1, G, backward)
    units(soon + 1, U - soon - 2, intra_grads)
    gr_part = ggrx.at[pl.ds(0, NC - 1)]
    remote(gr_part, gr_part, gr_s.at[0], gr_r.at[0], mate).wait()
    part = ggrx[0]
    for i in range(1, NC):
        part = part + ggrx[i]
    ggsum[...] = part
    ggall[chip] = part
    others(lambda i: remote(ggsum, ggall.at[chip], ga_s.at[0], ga_r.at[0], at(i)).start())

    def later_states(h):
        state = st[h]
        for j in range(NJ - 1, -1, -1):
            sbf[h, j] = state.astype(BF16)
            if j > 0:
                state = jnp.exp(cb[h, j * DH + DH - 1:j * DH + DH, :]) * state + ms[h, j]

    def last_mine(n):
        all_home(pin, gpi_s, gpi_r, n).wait_recv()
        settle(core == 1, pin, lpr, st, n)
        give(st, gps_s, gps_r, n, own0).start()

    def last_theirs(n):
        give(st, gps_s, gps_r, n, oth0).wait_recv()
        heads(oth0 + n * HG, later_states)

    loop(G, last_mine)
    units(U - 1, 1, intra_grads)
    loop(G, lambda n: heads(own0 + n * HG, later_states))
    loop(G, last_theirs)

    gg_part = ggall.at[pl.ds(0, NC - 1)]
    remote(gg_part, gg_part, ga_s.at[0], ga_r.at[0], mate).wait()
    for h in range(H):
        gg_out[h:h + 1, :] = jnp.sum(ggall[h], axis=0, keepdims=True)
    def done(n):
        all_out(rx, grx_s, grx_r, n).wait_send()
        all_back(gpi_s, gpi_r, n).wait_send()
        give(st, gps_s, gps_r, n, own0).wait_send()

    loop(G, done)


def on_device(sizes, queries, key_rows, value_rows, log_decay, norm_gain, grad_out):
    T, H, NC, NY = sizes
    W = H * DH
    NJ = T // DH
    HH = H // 2
    G = groups_of(HH)
    HG = HH // G
    RS = HG * DH // NC
    V = pltpu.VMEM
    D = pltpu.SemaphoreType.DMA
    rows = V((G, HG * DH, DH), F32)
    slots = V((G, NC, RS, DH), F32)
    heads = V((G, HG, DH, DH), F32)
    states = V((H, DH, DH), F32)
    scratch = [
        V((H, 1, T), F32), V((H, NJ, DH, DH), F32), V((T, W), BF16), V((T, W), BF16),
        V((T, W), BF16),
        V((T, DH), F32), V((T, DH), F32),
        V((8, T), F32), V((NY, 8, T), F32),
        V((H, 1, DH), F32), V((H, 1, DH), F32), V((H, 1, DH), F32), V((NC, H, 1, DH), F32),
        states, rows, slots, heads, heads, slots, rows, states,
        V((H, 8, DH), F32), V((H, 8, DH), F32), V((H, 8, DH), F32), V((NC, 8, DH), F32),
        V((8, DH), F32), V((NC, 8, DH), F32),
        D((6,)), *[D((1,))] * 6, *[D((G,))] * 16, *[D((1,))] * 6,
    ]
    anywhere = pl.BlockSpec(memory_space=pl.ANY)
    local = pl.BlockSpec(memory_space=V)
    held = (
        V((T, W), BF16), V((T, W), BF16), V((T, W), BF16), V((T, W), BF16),
        V((H, T, DH), F32), V((H, NJ, DH, DH), BF16), V((T, W), F32), V((T, W), F32),
        V((H, DH), F32),
    )
    parts = pl.pallas_call(
        functools.partial(kernel, sizes),
        out_shape=held,
        in_specs=[anywhere, anywhere, anywhere, local, local, anywhere],
        out_specs=(local,) * len(held),
        scratch_shapes=scratch,
        compiler_params=pltpu.CompilerParams(
            collective_id=0, has_side_effects=True, vmem_limit_bytes=23 << 20
        ),
    )(queries, key_rows, value_rows, log_decay, norm_gain.reshape(1, W), grad_out)
    parts = [pltpu.with_memory_space_constraint(x, V) for x in parts]
    big = jax.ShapeDtypeStruct((T, W), BF16)
    *grads, gain_grad = pl.pallas_call(
        functools.partial(finish, sizes),
        out_shape=(big, big, big, big, jax.ShapeDtypeStruct((H, DH), F32)),
        in_specs=[local] * len(held),
        out_specs=(anywhere, anywhere, anywhere, anywhere, local),
        scratch_shapes=[
            V((T, W), BF16), V((T, W), BF16), D((2,)), D((2, H)),
        ],
        compiler_params=pltpu.CompilerParams(vmem_limit_bytes=9 << 20),
    )(*parts)
    return (*grads, gain_grad.reshape(W))


def solution(mesh):
    def whole(queries, key_rows, value_rows, log_decay, norm_gain, grad_out):
        seq, head = mesh.shape["seq"], mesh.shape["head"]
        sizes = (queries.shape[0] // seq, queries.shape[1] // DH // head, seq // 2, head)
        rows = P("seq", "head")
        return jax.shard_map(
            functools.partial(on_device, sizes),
            mesh=mesh,
            in_specs=(rows, rows, rows, P("head", "seq"), P("head"), rows),
            out_specs=(rows, rows, rows, rows, P("head")),
            check_vma=False,
        )(queries, key_rows, value_rows, log_decay, norm_gain, grad_out)

    return whole
```
